32 devices in a mesh: ev: 2 (over core), own: 16 (over z, y, x).
Axes of the slice: x: 2, y: 2, z: 4, core: 2. Of those that a mesh axis runs over, the one named last changes fastest.
Arguments:
- ground_up: bfloat16 [8192, 4096], P('own', 'ev'), parts along dimension 1, may hold values from 0.049804688 to 2
- item_site: int32 [8192], P('own'), may hold values from 0 to 127
- item_profile: int32 [8192], P('own'), may hold values from 0 to 127
- site_owner: int32 [2048, 1], P('own'), may hold values from 0 to 15; in each aligned block of 128 rows (0 to 127, 128 to 255, ...) at most 16 rows name the same one
- site_slot: int32 [2048], P('own'), may hold values from 0 to 63
- site_profile: int32 [2048], P('own'), may hold values from 0 to 127
- policy_owner: int32 [1024, 1], P('own'), may hold values from 0 to 15; in each aligned block of 64 rows (0 to 63, 64 to 127, ...) at most 12 rows name the same one
- policy_slot: int32 [1024], P('own'), may hold values from 0 to 1
- policy_profile: int32 [1024], P('own'), may hold values from 0 to 127
- program_profile: int32 [32], P('own'), may hold values from 0 to 127
- term_table: float32 [4, 3, 128], replicated, may hold values from 0 to 90, as said below
Outputs:
- policy_loss: bfloat16 [1024, 4096], P('own', 'ev'), parts along dimension 1
- program_loss: float32 [32, 4096], P('own', 'ev'), parts along dimension 1
The draws below stay inside these ranges and needn't reach their ends.
There are 2 independent parts, one for each index of `ev`. The reference program is written for one: setup_inputs(seed, part) draws one part's arguments, and reference() takes and returns one part's arrays. A program takes and returns all parts, laid end to end along the dimension named above; an argument that names none is the same for every part. Nothing has to cross between parts.
Inputs may be any that keep to these rules, and one draw needn't show every extreme that they name: `site_owner`: among the 128 sites of one owner, no owner of policies appears more than 16 times; some owner appears exactly 16 times in some owner's sites. `policy_owner`: among the 64 policies of one owner, no owner of programs appears more than 12 times; some owner appears exactly 12 times in some owner's policies. `term_table`: deductibles are 0 or more, limits positive, shares between 0.5 and 1.
All inputs are finite; a program needn't handle non-finite values.
Results may differ from the reference program's by a relative error of at most 0.0051.
Values may be sent and summed in bfloat16 or wider, within the bound.
A program may use at most 64 MiB of HBM per device.

```python
import math
import jax
import jax.numpy as jnp
import numpy as np
from jax import lax

ROWS = 2048
ITEM_DEV = 512
SITE_DEV = 128
POL_DEV = 64
PROG_DEV = 2
PROFILES = 128
ITEMS = 8192
SITES = 2048
POLICIES = 1024
PROGRAMS = 32
CAP = 16
PROG_CAP = 12
N_OWN = 16


def draw_term_table(key, part):
    deduct_top = jnp.array([0.3, 1.0, 1.0, 20.0], jnp.float32)
    ceiling_low = jnp.array([0.5, 1.0, 2.0, 30.0], jnp.float32)
    ceiling_top = jnp.array([1.5, 4.0, 6.0, 90.0], jnp.float32)
    uniforms = jax.random.uniform(key, (4, 3, PROFILES), jnp.float32)
    deduct = uniforms[:, 0] * deduct_top[:, None]
    ceiling = ceiling_low[:, None] + uniforms[:, 1] * (ceiling_top - ceiling_low)[:, None]
    portion = 0.5 + 0.5 * uniforms[:, 2]
    return jnp.stack([deduct, ceiling, portion], axis=1)


def with_ends(values, key, least, largest):
    longest = values.shape.index(max(values.shape))
    spots = []
    for shift in (0, 1):
        where = [jax.random.randint(jax.random.fold_in(key, axis), (), 0, length) for axis, length in enumerate(values.shape)]
        where[longest] = (where[longest] + shift) % values.shape[longest]
        spots.append(tuple(where))
    return values.at[spots[0]].set(least).at[spots[1]].set(largest)


def block_scale(rng, shape, pieces, low, top_value):
    gain, own = 1.0, jax.random.fold_in(rng, 6)
    for dim, parts in pieces:
        steps = jnp.exp(jax.random.uniform(jax.random.fold_in(own, dim), (parts,), jnp.float32, low / len(pieces), top_value / len(pieces)))
        gain = gain * jnp.repeat(steps, shape[dim] // parts).reshape([-1 if axis == dim else 1 for axis in range(len(shape))])
    return gain


def rank_table(amount, lean):
    loads = [(1 << 20) // math.isqrt(standing ** lean) + 1 for standing in range(1, amount + 1)]
    width = 1 + sum(loads) // (1 << 30)
    return np.cumsum(np.array([max(1, weight // width) for weight in loads]))


def ranked(key, dims, number_of, skew):
    listing = rank_table(number_of, skew)
    ticket = jax.random.randint(jax.random.fold_in(key, 1), dims, 0, int(listing[number_of - 1]))
    rank = jnp.searchsorted(jnp.asarray(listing, jnp.int32), ticket, side="right")
    return jax.random.permutation(jax.random.fold_in(key, 2), number_of)[rank].astype(jnp.int32)


def shared_out(rng, own, number, rows, count, top, reach, skew):
    sequence = jax.random.permutation(rng, count)
    heavy_load, common = load_shares(count, rows * top, reach, skew, True), load_shares(count, rows * top, reach, skew, False)
    places = jnp.arange(count)

    def named(tallies, rotation):
        used = int((tallies > 0).sum())
        fixed = max(1, used // 4)
        shifted = fixed + (places - fixed + rotation * (used - fixed)) % max(1, count - fixed)
        return jnp.zeros((count,), jnp.int32).at[sequence[jnp.where(places < fixed, places, shifted)]].set(jnp.asarray(tallies, jnp.int32))

    tallies = jnp.where(number % 4 == 0, named(heavy_load, number // 4), named(common, number - number // 4 - 1))
    mixed = jax.random.permutation(jax.random.fold_in(own, 3), count)
    donor, taker = mixed[0:count // 2 * 2:2], mixed[1:count // 2 * 2:2]
    margin = jnp.minimum(tallies[donor] - 1, reach - tallies[taker]) // 2
    margin = jnp.where((donor == sequence[0]) | (taker == sequence[0]) | (tallies[taker] == 0), 0, jnp.maximum(margin, 0))
    shifted = jax.random.randint(jax.random.fold_in(own, 4), (count // 2,), 0, 1 << 20) % (margin + 1)
    tallies = tallies.at[donor].add(-shifted).at[taker].add(shifted)
    items = jnp.searchsorted(jnp.cumsum(tallies), jnp.arange(rows * top), side="right").astype(jnp.int32)
    listing = items.reshape(top, rows).T
    listing = listing[jax.random.permutation(jax.random.fold_in(own, 1), rows)]
    rotation = jax.random.randint(jax.random.fold_in(own, 2), (rows, 1), 0, top)
    return jnp.take_along_axis(listing, (jnp.arange(top)[None, :] + rotation) % top, axis=1)


def load_shares(number_of, total, reach, skew, full):
    weights = [(1 << 20) // math.isqrt(standing ** skew) + 1 for standing in range(1, number_of + 1)]
    largest = reach if full else min(reach, max(-(-total // number_of), total * weights[0] // sum(weights)))
    least = 1 if total - largest >= number_of - 1 else 0
    given, spare = [largest] + [least] * (number_of - 1), total - largest - least * (number_of - 1)
    while spare > 0:
        movable = [i for i in range(1, number_of) if given[i] < largest] or [i for i in range(1, number_of) if given[i] < reach]
        pool, remaining = sum([weights[i] for i in movable]), spare
        for i in movable:
            extra = min(reach - given[i], max(1, remaining * weights[i] // pool), spare)
            given[i] = given[i] + extra
            spare = spare - extra
    return np.array(given)


def setup_inputs(seed: int = 0, part: int = 0) -> dict:
    splits = jax.random.split(jax.random.key(seed), 12)
    own_keys = jax.random.split(jax.random.fold_in(splits[11], part), 12)
    ground_up = jnp.clip(jnp.exp(math.log(2.0) - 3.6927934 * jax.random.uniform(own_keys[0], (ITEMS, ROWS), jnp.float32) ** block_scale(own_keys[0], (ITEMS, ROWS), ((0, 16),), -0.2, 0.2)), 0.049804688, 2.0).astype(jnp.bfloat16)
    item_site = with_ends(ranked(splits[1], (ITEMS,), SITE_DEV, 1), jax.random.fold_in(splits[1], 3), 0, SITE_DEV - 1).astype(jnp.int32)
    item_profile = with_ends(jax.random.randint(splits[2], (ITEMS,), 0, PROFILES), jax.random.fold_in(splits[2], 1), 0, PROFILES - 1).astype(jnp.int32)
    site_owner_keys = jax.random.split(jax.random.fold_in(splits[3], 1), SITES // SITE_DEV)
    site_owner_turns = jax.random.permutation(jax.random.fold_in(splits[3], 3), SITES // SITE_DEV)
    site_owner = jax.vmap(lambda own, number: shared_out(jax.random.fold_in(splits[3], 2), own, number, SITE_DEV, N_OWN, 1, CAP, 2))(site_owner_keys, site_owner_turns).reshape((SITES, 1))
    site_slot = with_ends(jax.random.randint(splits[4], (SITES,), 0, POL_DEV), jax.random.fold_in(splits[4], 1), 0, POL_DEV - 1).astype(jnp.int32)
    site_profile = with_ends(jax.random.randint(splits[5], (SITES,), 0, PROFILES), jax.random.fold_in(splits[5], 1), 0, PROFILES - 1).astype(jnp.int32)
    policy_owner_keys = jax.random.split(jax.random.fold_in(splits[6], 1), POLICIES // POL_DEV)
    policy_owner_turns = jax.random.permutation(jax.random.fold_in(splits[6], 3), POLICIES // POL_DEV)
    policy_owner = jax.vmap(lambda own, number: shared_out(jax.random.fold_in(splits[6], 2), own, number, POL_DEV, N_OWN, 1, PROG_CAP, 2))(policy_owner_keys, policy_owner_turns).reshape((POLICIES, 1))
    policy_slot = with_ends(jax.random.randint(splits[7], (POLICIES,), 0, PROG_DEV), jax.random.fold_in(splits[7], 1), 0, PROG_DEV - 1).astype(jnp.int32)
    policy_profile = with_ends(jax.random.randint(splits[8], (POLICIES,), 0, PROFILES), jax.random.fold_in(splits[8], 1), 0, PROFILES - 1).astype(jnp.int32)
    program_profile = with_ends(jax.random.randint(splits[9], (PROGRAMS,), 0, PROFILES), jax.random.fold_in(splits[9], 1), 0, PROFILES - 1).astype(jnp.int32)
    term_table = draw_term_table(jax.random.fold_in(splits[11], 71), part)
    return dict(ground_up=ground_up, item_site=item_site, item_profile=item_profile, site_owner=site_owner, site_slot=site_slot, site_profile=site_profile, policy_owner=policy_owner, policy_slot=policy_slot, policy_profile=policy_profile, program_profile=program_profile, term_table=term_table)


def apply_terms(gross_loss, terms_table, tier_index, profile):
    deduct = terms_table[tier_index, 0][profile][:, None]
    ceiling = terms_table[tier_index, 1][profile][:, None]
    portion = terms_table[tier_index, 2][profile][:, None]
    return portion * jnp.minimum(jnp.maximum(gross_loss - deduct, 0.0), ceiling)


def reference(ground_up, item_site, item_profile, site_owner, site_slot, site_profile, policy_owner, policy_slot, policy_profile, program_profile, term_table):
    def site_block(inputs):
        losses, local_sites, profiles = inputs
        covered = apply_terms(losses.astype(jnp.float32), term_table, 0, profiles).astype(jnp.bfloat16)
        return jax.ops.segment_sum(covered.astype(jnp.float32), local_sites, num_segments=SITE_DEV)

    site_gross = lax.map(site_block, (ground_up.reshape(N_OWN, ITEM_DEV, ROWS), item_site.reshape(N_OWN, ITEM_DEV), item_profile.reshape(N_OWN, ITEM_DEV)))
    site_gross = site_gross.reshape(SITES, ROWS)
    site_net = apply_terms(site_gross, term_table, 1, site_profile).astype(jnp.bfloat16)
    policy_ids = (site_owner[:, 0] * POL_DEV + site_slot).astype(jnp.int32)
    policy_gross = jax.ops.segment_sum(site_net.astype(jnp.float32), policy_ids, num_segments=POLICIES)
    policy_loss = apply_terms(policy_gross, term_table, 2, policy_profile).astype(jnp.bfloat16)
    program_ids = (policy_owner[:, 0] * PROG_DEV + policy_slot).astype(jnp.int32)
    program_gross = jax.ops.segment_sum(policy_loss.astype(jnp.float32), program_ids, num_segments=PROGRAMS)
    program_loss = apply_terms(program_gross, term_table, 3, program_profile)
    return (policy_loss, program_loss)
```

```python
import functools

import jax
import jax.numpy as jnp
from jax import lax
from jax.experimental import pallas as pl
from jax.experimental.pallas import tpu as pltpu
from jax.sharding import PartitionSpec as P

LANES = 128
SMALL = 10
f32 = jnp.float32
bf16 = jnp.bfloat16


def terms(x, deduct, ceiling, portion):
    return portion * jnp.minimum(jnp.maximum(x - deduct, 0.0), ceiling)


def mixed(a, b, n):
    d, bit = 0, 1
    while bit < n:
        d = d + bit * lax.rem(lax.div(a, bit) + lax.div(b, bit), 2)
        bit *= 2
    return d


def kernel(
    n,
    pol,
    prog,
    ground,
    *refs,
):
    small_in, refs = refs[:SMALL], refs[SMALL:]
    policy_out, program_out = refs[:2]
    (
        item_rows,
        site_rows,
        policy_rows,
        program_row,
        table,
        chunks,
        ids,
        square,
        item_terms,
        site_terms,
        policy_terms,
        program_terms,
        grouping,
        meta,
        near_send,
        near_recv,
        full_send,
        full_recv,
        part_send,
        part_recv,
        near_acc,
        near_losses,
        full_losses,
        full_policy,
        program_send,
        program_recv,
        marks,
        picks,
        small_sem,
        load_sem,
        part_rs,
        sends,
        recvs,
    ) = refs[2:]
    me = lax.axis_index("own")
    team = n // 2
    side = lax.div(me, team)
    seat = lax.rem(me, team)
    base = side * team
    other = (1 - side) * team
    mate = other + seat
    items = ground.shape[0]
    blocks = items // LANES
    sites = near_send.shape[1]
    width = near_send.shape[2]
    wide = 2 * width
    rows = team * pol
    META, NEAR, FULL, PART, NEAR_POLICY, FULL_POLICY, PROGRAM = range(7)

    def turn(i):
        return mixed(seat, lax.rem(i + 1, team), team)

    barrier = pltpu.get_barrier_semaphore()

    def greet(k, c):
        pl.semaphore_signal(barrier, inc=1, device_id={"own": lax.rem(me + k, n)})
        return c

    homes = (
        [item_rows.at[pl.ds(i * blocks, blocks), :] for i in range(2)]
        + [site_rows.at[pl.ds(i, 1), :] for i in range(3)]
        + [policy_rows.at[pl.ds(i, 1), :] for i in range(3)]
        + [program_row, table]
    )
    for i, (src, dst) in enumerate(zip(small_in, homes)):
        pltpu.make_async_copy(src, dst, small_sem.at[(0, 0, 1, 1, 1, 2, 2, 2, 3, 4)[i]]).start()

    lax.fori_loop(1, n, greet, 0)

    def load(i):
        return pltpu.make_async_copy(
            ground.at[:, pl.ds(pl.multiple_of(turn(i) * wide, wide), wide)],
            chunks.at[i],
            load_sem.at[i],
        )

    def start_load(i, c):
        load(i).start()
        return c

    lax.fori_loop(0, team, start_load, 0)
    with jax.named_scope("small"):
        for i, whole in enumerate((item_rows, site_rows, policy_rows, program_row, table)):
            pltpu.make_async_copy(whole, whole, small_sem.at[i]).wait()

    square[...] = jnp.zeros_like(square)
    for t in range(3):
        square[4 * t : 4 * t + 4, :] = table[t]
    columns = square[...].T
    rows_iota = lax.broadcasted_iota(jnp.int32, (LANES, LANES), 0)

    def look(profile_row, level):
        pick = rows_iota == profile_row
        return [
            jnp.sum(
                jnp.where(pick, columns[:, 4 * t + level : 4 * t + level + 1], 0.0),
                axis=0,
                keepdims=True,
            )
            for t in range(3)
        ]

    with jax.named_scope("prep"):
        ids[...] = jnp.zeros_like(ids)
        ids[0:1, 0:pol] = policy_rows[2:3, :]
        ids[0:1, pol : 2 * pol] = policy_rows[0:1, :] * prog + policy_rows[1:2, :]
        ids[1:2, 0:prog] = program_row[...]
        meta[me] = jnp.concatenate([site_rows[0:1, :] * pol + site_rows[1:2, :], ids[0:1, :]], axis=0)

        for b in range(blocks):
            grouping[:, b * LANES : (b + 1) * LANES] = (rows_iota == item_rows[b : b + 1, :]).astype(bf16)
            for t, row in enumerate(look(item_rows[blocks + b : blocks + b + 1, :], 0)):
                square[3 * b + t : 3 * b + t + 1, :] = row
        for t, row in enumerate(look(site_rows[2:3, :], 1)):
            square[3 * blocks + t : 3 * blocks + t + 1, :] = row
        for t, row in enumerate(look(ids[1:2, :], 3)):
            square[3 * blocks + 3 + t : 3 * blocks + 4 + t, :] = row
        flipped = square[...].T
        for t in range(3):
            for b in range(blocks):
                item_terms[t, b * LANES : (b + 1) * LANES, :] = jnp.broadcast_to(
                    flipped[:, 3 * b + t : 3 * b + t + 1], (LANES, LANES)
                )
            program_terms[t] = jnp.broadcast_to(
                flipped[0:prog, 3 * blocks + 3 + t : 3 * blocks + 4 + t], (prog, LANES)
            )
            site_terms[t] = jnp.broadcast_to(
                flipped[:, 3 * blocks + t : 3 * blocks + t + 1], (LANES, LANES)
            )

    def remote(kind, src, dst, d):
        return pltpu.make_async_remote_copy(src, dst, sends.at[kind], recvs.at[kind], device_id={"own": d})

    def columns_of(block):
        return pl.ds(pl.multiple_of(block * width, width), width)

    def rows_of(q, count):
        return pl.ds(pl.multiple_of(q * count, count), count)

    def meta_copy(d):
        return remote(META, meta.at[me], meta.at[me], d)

    def near_copy(g):
        return remote(NEAR, near_send.at[g], near_recv.at[seat], base + g)

    def full_copy(d):
        return remote(FULL, full_send.at[d], full_recv.at[me], d)

    def part_copy(q):
        return pltpu.make_async_remote_copy(
            part_send.at[q], part_recv.at[q], sends.at[PART], part_rs.at[q], device_id={"own": mate}
        )

    def near_policy_copy(q):
        return remote(
            NEAR_POLICY, near_losses.at[rows_of(q, pol), :], policy_out.at[:, columns_of(2 * seat)], base + q
        )

    def full_policy_copy(d):
        return remote(FULL_POLICY, full_losses.at[d], full_policy.at[me], d)

    def program_copy(d):
        return remote(PROGRAM, program_send.at[d], program_recv.at[me], d)

    def bulk(kind, ref):
        return remote(kind, ref, ref, me)

    def others(fn):
        def step(k, c):
            fn(mixed(me, n - k, n))
            return c

        lax.fori_loop(1, n, step, 0)

    def loop(start, stop, fn):
        def step(i, c):
            fn(i)
            return c

        lax.fori_loop(start, stop, step, 0)

    def spread_of(refs_terms, at, count):
        return [jnp.concatenate([refs_terms[t, at, :]] * count, axis=1) for t in range(3)]

    every = slice(None)
    low_half = lax.broadcasted_iota(jnp.int32, (sites // 2, width), 1) < width // 2

    def swap(x):
        return pltpu.roll(x, width // 2, x.ndim - 1)

    def site_losses(i):
        load(i).wait()
        g = turn(i)
        covered = terms(chunks[i].astype(f32), *spread_of(item_terms, every, wide // LANES)).astype(bf16)
        gross = jnp.dot(grouping[...], covered, preferred_element_type=f32)
        net = terms(gross, *spread_of(site_terms, every, wide // LANES))
        near = net[:, :width].astype(bf16)
        top, bottom = net[: sites // 2, width:], net[sites // 2 :, width:]
        left = jnp.where(low_half, top, swap(bottom)).astype(bf16)
        right = jnp.where(low_half, swap(top), bottom).astype(bf16)
        ours = jnp.where(side == 0, left, right)
        theirs = jnp.where(side == 0, right, left)
        full_send[other + g] = theirs

        @pl.when(g == seat)
        def _():
            near_recv[seat] = near
            full_recv[me] = ours

        @pl.when(g != seat)
        def _():
            near_send[g] = near
            full_send[base + g] = ours

    lag = team // 2

    def send_near(i):
        near_copy(turn(i)).start()

    def send_cross(i):
        full_copy(other + turn(i)).start()

    with jax.named_scope("first"):
        site_losses(0)
    with jax.named_scope("bar"):
        pl.semaphore_wait(barrier, n - 1)
    with jax.named_scope("sites"):
        others(lambda d: meta_copy(d).start())

        def near_step(i):
            site_losses(i)
            send_near(i)

        def mixed_step(i):
            site_losses(i)
            send_near(i)
            send_cross(i - lag)

        send_near(0)
        loop(1, lag, near_step)
        loop(lag, team - 1, mixed_step)
        site_losses(team - 1)
        loop(lag - 1, team, send_cross)
        loop(0, team - 1, lambda i: full_copy(base + turn(i)).start())
    with jax.named_scope("metawait"):
        bulk(META, meta.at[pl.ds(0, n - 1)]).wait_recv()

    policy_iota = lax.broadcasted_iota(jnp.int32, (n * pol, sites), 0)
    program_iota = lax.broadcasted_iota(jnp.int32, (n * prog, pol), 0)

    def learn(start):
        for o in range(team):
            for t, row in enumerate(look(meta[start + o][1:2, :], 2)):
                square[3 * o + t : 3 * o + t + 1, :] = row
        turned = square[...].T
        for o in range(team):
            for t in range(3):
                lane = 3 * o + t
                policy_terms[t, rows_of(start + o, pol), :] = jnp.broadcast_to(
                    turned[0:pol, lane : lane + 1], (pol, LANES)
                )
        which = lax.div(start, team)
        marks[which] = jnp.concatenate(
            [(program_iota == meta[start + o][1:2, pol : 2 * pol]).astype(bf16) for o in range(team)], axis=1
        )
        for o in range(team):
            picks[which, :, o * sites : (o + 1) * sites] = (policy_iota == meta[start + o][0:1, :]).astype(bf16)

    with jax.named_scope("learn"):
        learn(base)
    with jax.named_scope("nearwait"):
        bulk(NEAR, near_recv.at[pl.ds(0, team - 1)]).wait_recv()
    ours_at, theirs_at = (pl.ds(pl.multiple_of(h * pol, rows), rows) for h in (base, other))

    def near_sum(at):
        return jnp.dot(
            picks[side, at, :], near_recv[...].reshape(team * sites, width), preferred_element_type=f32
        )

    with jax.named_scope("nearsum"):
        part_send[...] = near_sum(theirs_at).astype(bf16).reshape(team, pol, width)
        loop(0, team, lambda i: part_copy(turn(i)).start())
    with jax.named_scope("nearsum2"):
        near_acc[...] = near_sum(ours_at)
    with jax.named_scope("learn2"):
        learn(other)
    with jax.named_scope("fullwait"):
        bulk(FULL, full_recv.at[pl.ds(0, n - 1)]).wait_recv()
    with jax.named_scope("fullsum"):

        def unpacked(k):
            packed = full_recv[k * team : (k + 1) * team]
            return jnp.concatenate([packed, swap(packed)], axis=1).reshape(team * sites, width)

        total = jnp.dot(picks[0], unpacked(0), preferred_element_type=f32) + jnp.dot(
            picks[1], unpacked(1), preferred_element_type=f32
        )
        loss = terms(total, *spread_of(policy_terms, every, width // LANES))
        split = loss.reshape(n, 2, pol // 2, width)
        mask = lax.broadcasted_iota(jnp.int32, (n, pol // 2, width), 2) < width // 2
        full_losses[...] = jnp.where(mask, split[:, 0], swap(split[:, 1])).astype(bf16)
        others(lambda d: full_policy_copy(d).start())
        full_policy[me] = full_losses[me]
        loss = loss.astype(bf16)
        gross = jnp.dot(marks[0], loss[0:rows], preferred_element_type=f32) + jnp.dot(
            marks[1], loss[rows : 2 * rows], preferred_element_type=f32
        )
        for o in range(n):
            program_send[o, 1] = gross[o * prog : (o + 1) * prog, :]

    def close(i):
        q = turn(i)
        part_copy(q).wait_recv()
        at = rows_of(base + q, pol)
        gross = near_acc[rows_of(q, pol), :] + part_recv[q].astype(f32)
        loss = terms(gross, *spread_of(policy_terms, at, width // LANES)).astype(bf16)
        near_losses[rows_of(q, pol), :] = loss

        @pl.when(q != seat)
        def _():
            near_policy_copy(q).start()

        @pl.when(q == seat)
        def _():
            policy_out[:, columns_of(2 * seat)] = loss

    with jax.named_scope("close"):
        loop(0, team, close)
    with jax.named_scope("progsend"):
        near_gross = jnp.dot(marks[side], near_losses[...], preferred_element_type=f32)
        for o in range(n):
            program_send[o, 0] = near_gross[o * prog : (o + 1) * prog, :]
        others(lambda d: program_copy(d).start())
        program_recv[me] = program_send[me]
    with jax.named_scope("fpolwait"):
        bulk(FULL_POLICY, full_policy.at[pl.ds(0, n - 1)]).wait_recv()
        low = lax.broadcasted_iota(jnp.int32, (pol // 2, width), 1) < width // 2
        for g in range(team):
            left, right = full_policy[g].astype(f32), full_policy[team + g].astype(f32)
            at = slice((2 * g + 1) * width, (2 * g + 2) * width)
            policy_out[: pol // 2, at] = jnp.where(low, left, swap(right)).astype(bf16)
            policy_out[pol // 2 :, at] = jnp.where(low, swap(left), right).astype(bf16)
    with jax.named_scope("sent"):
        bulk(META, meta.at[pl.ds(0, n - 1)]).wait_send()
        bulk(NEAR, near_send.at[pl.ds(0, team - 1)]).wait_send()
        bulk(FULL, full_send.at[pl.ds(0, n - 1)]).wait_send()
        bulk(PART, part_send).wait_send()
        bulk(NEAR_POLICY, near_losses.at[pl.ds(0, rows - pol), :]).wait_send()
        bulk(FULL_POLICY, full_losses.at[pl.ds(0, n - 1)]).wait_send()
        bulk(PROGRAM, program_send.at[pl.ds(0, n - 1)]).wait_send()
    with jax.named_scope("npolwait"):
        bulk(NEAR_POLICY, near_losses.at[pl.ds(0, rows - pol), :]).wait_recv()
    with jax.named_scope("progwait"):
        bulk(PROGRAM, program_recv.at[pl.ds(0, n - 1)]).wait_recv()
    with jax.named_scope("tail"):
        spread = spread_of(program_terms, every, width // LANES)
        low = lax.broadcasted_iota(jnp.int32, (prog, width), 1) < width // 2
        for g in range(team):
            near = program_recv[g, 0] + program_recv[team + g, 0]
            full = jnp.where(low, program_recv[g, 1], swap(program_recv[team + g, 1]))
            at = 2 * g * width
            program_out[:, at : at + width] = terms(near, *spread)
            program_out[:, at + width : at + 2 * width] = terms(full, *spread)


def exchange(
    ground_up,
    item_site,
    item_profile,
    site_owner,
    site_slot,
    site_profile,
    policy_owner,
    policy_slot,
    policy_profile,
    program_profile,
    term_table,
):
    n = lax.axis_size("own")
    items, cols = ground_up.shape
    sites = site_profile.shape[0]
    pol = policy_profile.shape[0]
    prog = program_profile.shape[0]
    width = cols // n
    team = n // 2

    def row(v):
        return v.reshape(-1, min(v.size, LANES))

    inputs = [
        row(v)
        for v in (
            item_site,
            item_profile,
            site_owner,
            site_slot,
            site_profile,
            policy_owner,
            policy_slot,
            policy_profile,
            program_profile,
        )
    ] + [term_table.transpose(1, 0, 2)]
    vmemspec = pl.BlockSpec(memory_space=pltpu.VMEM)
    anyspec = pl.BlockSpec(memory_space=pl.ANY)
    dma = pltpu.SemaphoreType.DMA
    return pl.pallas_call(
        functools.partial(kernel, n, pol, prog),
        out_shape=(
            pltpu.VMEM((pol, cols), bf16),
            pltpu.VMEM((prog, cols), f32),
        ),
        in_specs=[anyspec] * (1 + SMALL),
        out_specs=(vmemspec, vmemspec),
        scratch_shapes=[
            pltpu.VMEM((2 * (items // LANES), LANES), jnp.int32),
            pltpu.VMEM((3, sites), jnp.int32),
            pltpu.VMEM((3, pol), jnp.int32),
            pltpu.VMEM((1, prog), jnp.int32),
            pltpu.VMEM(inputs[-1].shape, f32),
            pltpu.VMEM((team, items, 2 * width), bf16),
            pltpu.VMEM((8, LANES), jnp.int32),
            pltpu.VMEM((LANES, LANES), f32),
            pltpu.VMEM((3, items, LANES), f32),
            pltpu.VMEM((3, sites, LANES), f32),
            pltpu.VMEM((3, n * pol, LANES), f32),
            pltpu.VMEM((3, prog, LANES), f32),
            pltpu.VMEM((sites, items), bf16),
            pltpu.VMEM((n, 2, LANES), jnp.int32),
            pltpu.VMEM((team, sites, width), bf16),
            pltpu.VMEM((team, sites, width), bf16),
            pltpu.VMEM((n, sites // 2, width), bf16),
            pltpu.VMEM((n, sites // 2, width), bf16),
            pltpu.VMEM((team, pol, width), bf16),
            pltpu.VMEM((team, pol, width), bf16),
            pltpu.VMEM((team * pol, width), f32),
            pltpu.VMEM((team * pol, width), bf16),
            pltpu.VMEM((n, pol // 2, width), bf16),
            pltpu.VMEM((n, pol // 2, width), bf16),
            pltpu.VMEM((n, 2, prog, width), f32),
            pltpu.VMEM((n, 2, prog, width), f32),
            pltpu.VMEM((2, n * prog, team * pol), bf16),
            pltpu.VMEM((2, n * pol, team * sites), bf16),
            dma((5,)),
            dma((team,)),
            dma((team,)),
            dma((7,)),
            dma((7,)),
        ],
        compiler_params=pltpu.CompilerParams(collective_id=0, has_side_effects=True),
        name="loss_terms",
    )(ground_up, *inputs)


def apply_terms(gross_loss, terms_table, tier_index, profile):
    profile_iota = jnp.arange(terms_table.shape[2], dtype=jnp.int32)
    picker = profile[:, None] == profile_iota[None, :]
    deduct = jnp.sum(jnp.where(picker, terms_table[tier_index, 0][None, :], 0.0), axis=1)[:, None]
    ceiling = jnp.sum(jnp.where(picker, terms_table[tier_index, 1][None, :], 0.0), axis=1)[:, None]
    portion = jnp.sum(jnp.where(picker, terms_table[tier_index, 2][None, :], 0.0), axis=1)[:, None]
    return portion * jnp.minimum(jnp.maximum(gross_loss - deduct, 0.0), ceiling)


def pack_rows(values, target_dev, inner_slot, owners, capacity):
    member = (target_dev[:, None] == jnp.arange(owners, dtype=jnp.int32)[None, :]).astype(jnp.int32)
    before = jnp.cumsum(member, axis=0) - member
    position = jnp.sum(before * member, axis=1)
    target = target_dev * capacity + position
    placer = jnp.arange(owners * capacity, dtype=jnp.int32)[:, None] == target[None, :]
    packed = jnp.dot(
        placer.astype(jnp.bfloat16), values, preferred_element_type=jnp.float32
    ).astype(jnp.bfloat16)
    labels = jnp.sum(jnp.where(placer, (inner_slot + 1)[None, :], 0), axis=1) - 1
    return (
        packed.reshape(owners, capacity, values.shape[1]),
        labels.astype(jnp.bfloat16).reshape(owners, capacity),
    )


def sum_rows(received, labels, slot_count):
    flattened = received.reshape(-1, received.shape[2])
    slot_marks = labels.reshape(-1).astype(jnp.int32)
    picker = (jnp.arange(slot_count, dtype=jnp.int32)[:, None] == slot_marks[None, :]).astype(
        jnp.bfloat16
    )
    return jnp.dot(picker, flattened, preferred_element_type=jnp.float32)


def shards(
    ground_up,
    item_site,
    item_profile,
    site_owner,
    site_slot,
    site_profile,
    policy_owner,
    policy_slot,
    policy_profile,
    program_profile,
    term_table,
):
    owners = lax.axis_size("own")
    covered = apply_terms(ground_up.astype(jnp.float32), term_table, 0, item_profile).astype(
        jnp.bfloat16
    )
    site_total = site_profile.shape[0]
    grouping = (jnp.arange(site_total, dtype=jnp.int32)[:, None] == item_site[None, :]).astype(
        jnp.bfloat16
    )
    site_gross = jnp.dot(grouping, covered, preferred_element_type=jnp.float32)
    site_net = apply_terms(site_gross, term_table, 1, site_profile).astype(jnp.bfloat16)
    capacity = 2 * site_total // owners
    packed, labels = pack_rows(site_net, site_owner[:, 0], site_slot, owners, capacity)
    arrived, arrived_labels = (
        lax.all_to_all(packed, "own", split_axis=0, concat_axis=0, tiled=True),
        lax.all_to_all(labels, "own", split_axis=0, concat_axis=0, tiled=True),
    )
    policy_total = policy_profile.shape[0]
    policy_gross = sum_rows(arrived, arrived_labels, policy_total)
    policy_loss = apply_terms(policy_gross, term_table, 2, policy_profile).astype(jnp.bfloat16)
    program_total = program_profile.shape[0]
    program_capacity = 3 * policy_total // owners
    sent_rows, sent_labels = pack_rows(
        policy_loss, policy_owner[:, 0], policy_slot, owners, program_capacity
    )
    got_rows, got_labels = (
        lax.all_to_all(sent_rows, "own", split_axis=0, concat_axis=0, tiled=True),
        lax.all_to_all(sent_labels, "own", split_axis=0, concat_axis=0, tiled=True),
    )
    program_gross = sum_rows(got_rows, got_labels, program_total)
    program_loss = apply_terms(program_gross, term_table, 3, program_profile)
    return (policy_loss, program_loss)


def solution(mesh):
    placed = (
        P("own", "ev"),
        P("own"),
        P("own"),
        P("own", None),
        P("own"),
        P("own"),
        P("own", None),
        P("own"),
        P("own"),
        P("own"),
        P(),
    )

    def body(ground_up, item_site, item_profile, *rest):
        n = lax.axis_size("own")
        items, cols = ground_up.shape
        sites, pol = rest[2].shape[0], rest[5].shape[0]
        prog = rest[6].shape[0]
        fits = cols % (n * LANES) == 0 and items % LANES == 0 and sites == LANES
        fits = fits and 2 * pol <= LANES and pol % 16 == 0 and prog <= 8
        fits = fits and n % 4 == 0 and n & (n - 1) == 0 and 3 * n <= LANES and 3 * items <= LANES * (LANES - 6)
        return (exchange if fits else shards)(ground_up, item_site, item_profile, *rest)

    return jax.shard_map(
        body,
        mesh=mesh,
        in_specs=placed,
        out_specs=(P("own", "ev"), P("own", "ev")),
        check_vma=False,
    )
```

```python
import functools

import jax
import jax.numpy as jnp
from jax import lax
from jax.experimental import pallas as pl
from jax.experimental.pallas import tpu as pltpu
from jax.sharding import PartitionSpec as P

LANES = 128
SMALL = 10
f32 = jnp.float32
bf16 = jnp.bfloat16


def terms(x, deduct, ceiling, portion):
    return portion * jnp.minimum(jnp.maximum(x - deduct, 0.0), ceiling)


def mixed(a, b, n):
    d, bit = 0, 1
    while bit < n:
        d = d + bit * lax.rem(lax.div(a, bit) + lax.div(b, bit), 2)
        bit *= 2
    return d


def kernel(
    n,
    pol,
    prog,
    ground,
    *refs,
):
    small_in, refs = refs[:SMALL], refs[SMALL:]
    policy_out, program_out = refs[:2]
    (
        item_rows,
        site_rows,
        policy_rows,
        program_row,
        table,
        chunks,
        ids,
        square,
        item_terms,
        site_terms,
        policy_terms,
        program_terms,
        grouping,
        meta,
        near_send,
        near_recv,
        full_send,
        full_recv,
        part_send,
        part_recv,
        near_acc,
        near_losses,
        full_losses,
        full_policy,
        program_send,
        program_recv,
        marks,
        picks,
        small_sem,
        load_sem,
        part_rs,
        sends,
        recvs,
    ) = refs[2:]
    me = lax.axis_index("own")
    team = n // 2
    side = lax.div(me, team)
    seat = lax.rem(me, team)
    base = side * team
    other = (1 - side) * team
    mate = other + seat
    items = ground.shape[0]
    blocks = items // LANES
    sites = near_send.shape[1]
    width = near_send.shape[2]
    wide = 2 * width
    rows = team * pol
    META, NEAR, FULL, PART, NEAR_POLICY, FULL_POLICY, PROGRAM = range(7)

    def turn(i):
        half = team // 2
        late = lax.div(i, half)
        return mixed(seat, (1 - late) * (i + half) + late * lax.rem(i + 1, half), team)

    barrier = pltpu.get_barrier_semaphore()

    def greet(k, c):
        pl.semaphore_signal(barrier, inc=1, device_id={"own": lax.rem(me + k, n)})
        return c

    homes = (
        [item_rows.at[pl.ds(i * blocks, blocks), :] for i in range(2)]
        + [site_rows.at[pl.ds(i, 1), :] for i in range(3)]
        + [policy_rows.at[pl.ds(i, 1), :] for i in range(3)]
        + [program_row, table]
    )
    for i, (src, dst) in enumerate(zip(small_in, homes)):
        pltpu.make_async_copy(src, dst, small_sem.at[(0, 0, 1, 1, 1, 2, 2, 2, 3, 4)[i]]).start()

    lax.fori_loop(1, n, greet, 0)

    def load(i):
        return pltpu.make_async_copy(
            ground.at[:, pl.ds(pl.multiple_of(turn(i) * wide, wide), wide)],
            chunks.at[i],
            load_sem.at[i],
        )

    def start_load(i, c):
        load(i).start()
        return c

    lax.fori_loop(0, team, start_load, 0)
    with jax.named_scope("small"):
        for i, whole in enumerate((item_rows, site_rows, policy_rows, program_row, table)):
            pltpu.make_async_copy(whole, whole, small_sem.at[i]).wait()

    square[...] = jnp.zeros_like(square)
    for t in range(3):
        square[4 * t : 4 * t + 4, :] = table[t]
    columns = square[...].T
    rows_iota = lax.broadcasted_iota(jnp.int32, (LANES, LANES), 0)

    def look(profile_row, level):
        pick = rows_iota == profile_row
        return [
            jnp.sum(
                jnp.where(pick, columns[:, 4 * t + level : 4 * t + level + 1], 0.0),
                axis=0,
                keepdims=True,
            )
            for t in range(3)
        ]

    with jax.named_scope("prep"):
        ids[...] = jnp.zeros_like(ids)
        ids[0:1, 0:pol] = policy_rows[2:3, :]
        ids[0:1, pol : 2 * pol] = policy_rows[0:1, :] * prog + policy_rows[1:2, :]
        ids[1:2, 0:prog] = program_row[...]
        meta[me] = jnp.concatenate([site_rows[0:1, :] * pol + site_rows[1:2, :], ids[0:1, :]], axis=0)

        for b in range(blocks):
            grouping[:, b * LANES : (b + 1) * LANES] = (rows_iota == item_rows[b : b + 1, :]).astype(bf16)
            for t, row in enumerate(look(item_rows[blocks + b : blocks + b + 1, :], 0)):
                square[3 * b + t : 3 * b + t + 1, :] = row
        for t, row in enumerate(look(site_rows[2:3, :], 1)):
            square[3 * blocks + t : 3 * blocks + t + 1, :] = row
        for t, row in enumerate(look(ids[1:2, :], 3)):
            square[3 * blocks + 3 + t : 3 * blocks + 4 + t, :] = row
        flipped = square[...].T
        for t in range(3):
            for b in range(blocks):
                item_terms[t, b * LANES : (b + 1) * LANES, :] = jnp.broadcast_to(
                    flipped[:, 3 * b + t : 3 * b + t + 1], (LANES, LANES)
                )
            program_terms[t] = jnp.broadcast_to(
                flipped[0:prog, 3 * blocks + 3 + t : 3 * blocks + 4 + t], (prog, LANES)
            )
            site_terms[t] = jnp.broadcast_to(
                flipped[:, 3 * blocks + t : 3 * blocks + t + 1], (LANES, LANES)
            )

    def remote(kind, src, dst, d):
        return pltpu.make_async_remote_copy(src, dst, sends.at[kind], recvs.at[kind], device_id={"own": d})

    def columns_of(block):
        return pl.ds(pl.multiple_of(block * width, width), width)

    def rows_of(q, count):
        return pl.ds(pl.multiple_of(q * count, count), count)

    def meta_copy(d):
        return remote(META, meta.at[me], meta.at[me], d)

    def near_copy(g):
        return remote(NEAR, near_send.at[g], near_recv.at[seat], base + g)

    def full_copy(d):
        return remote(FULL, full_send.at[d], full_recv.at[me], d)

    def part_copy(q):
        return pltpu.make_async_remote_copy(
            part_send.at[q], part_recv.at[q], sends.at[PART], part_rs.at[q], device_id={"own": mate}
        )

    def near_policy_copy(q):
        return remote(
            NEAR_POLICY, near_losses.at[rows_of(q, pol), :], policy_out.at[:, columns_of(2 * seat)], base + q
        )

    def full_policy_copy(d):
        return remote(FULL_POLICY, full_losses.at[d], full_policy.at[me], d)

    def program_copy(d):
        return remote(PROGRAM, program_send.at[d], program_recv.at[me], d)

    def bulk(kind, ref):
        return remote(kind, ref, ref, me)

    def others(fn):
        def step(k, c):
            fn(mixed(me, n - k, n))
            return c

        lax.fori_loop(1, n, step, 0)

    def loop(start, stop, fn):
        def step(i, c):
            fn(i)
            return c

        lax.fori_loop(start, stop, step, 0)

    def spread_of(refs_terms, at, count):
        return [jnp.concatenate([refs_terms[t, at, :]] * count, axis=1) for t in range(3)]

    every = slice(None)
    low_half = lax.broadcasted_iota(jnp.int32, (sites // 2, width), 1) < width // 2

    def swap(x):
        return pltpu.roll(x, width // 2, x.ndim - 1)

    def site_losses(i):
        load(i).wait()
        g = turn(i)
        covered = terms(chunks[i].astype(f32), *spread_of(item_terms, every, wide // LANES)).astype(bf16)
        gross = jnp.dot(grouping[...], covered, preferred_element_type=f32)
        net = terms(gross, *spread_of(site_terms, every, wide // LANES))
        near = net[:, :width].astype(bf16)
        top, bottom = net[: sites // 2, width:], net[sites // 2 :, width:]
        left = jnp.where(low_half, top, swap(bottom)).astype(bf16)
        right = jnp.where(low_half, swap(top), bottom).astype(bf16)
        ours = jnp.where(side == 0, left, right)
        theirs = jnp.where(side == 0, right, left)
        full_send[other + g] = theirs

        @pl.when(g == seat)
        def _():
            near_recv[seat] = near
            full_recv[me] = ours

        @pl.when(g != seat)
        def _():
            near_send[g] = near
            full_send[base + g] = ours

    lag = team // 2
    inner = lax.rem(lax.div(seat, lag) + side, 2)

    def send_near(i):
        near_copy(turn(i)).start()

    def send_cross(i):
        full_copy(other + turn(i)).start()

    plane, corner = lax.div(me, 4), lax.rem(me, 4)
    hops = plane + lax.div(corner, 2) + lax.rem(corner, 2)
    ahead = lax.clamp(1, 13 - 3 * hops, team - 1)
    with jax.named_scope("first"):
        loop(0, ahead, site_losses)
    with jax.named_scope("bar"):
        pl.semaphore_wait(barrier, n - 1)
    with jax.named_scope("sites"):
        others(lambda d: meta_copy(d).start())

        def send(i):
            send_near(i)
            @pl.when(inner == 1)
            def _():
                send_cross(i)

            @pl.when((inner == 0) & (i >= lag))
            def _():
                send_cross(i - lag)

        def step(i):
            site_losses(i)
            send(i)

        loop(0, ahead, send)
        loop(ahead, team - 1, step)
        site_losses(team - 1)
        loop(lax.select(inner == 1, team - 1, lag - 1), team, send_cross)
        loop(0, team - 1, lambda i: full_copy(base + turn(i)).start())
    with jax.named_scope("metawait"):
        bulk(META, meta.at[pl.ds(0, n - 1)]).wait_recv()

    policy_iota = lax.broadcasted_iota(jnp.int32, (n * pol, sites), 0)
    program_iota = lax.broadcasted_iota(jnp.int32, (n * prog, pol), 0)

    def learn(start):
        for o in range(team):
            for t, row in enumerate(look(meta[start + o][1:2, :], 2)):
                square[3 * o + t : 3 * o + t + 1, :] = row
        turned = square[...].T
        for o in range(team):
            for t in range(3):
                lane = 3 * o + t
                policy_terms[t, rows_of(start + o, pol), :] = jnp.broadcast_to(
                    turned[0:pol, lane : lane + 1], (pol, LANES)
                )
        which = lax.div(start, team)
        marks[which] = jnp.concatenate(
            [(program_iota == meta[start + o][1:2, pol : 2 * pol]).astype(bf16) for o in range(team)], axis=1
        )
        for o in range(team):
            picks[which, :, o * sites : (o + 1) * sites] = (policy_iota == meta[start + o][0:1, :]).astype(bf16)

    with jax.named_scope("learn"):
        learn(base)
    with jax.named_scope("nearwait"):
        bulk(NEAR, near_recv.at[pl.ds(0, team - 1)]).wait_recv()
    ours_at, theirs_at = (pl.ds(pl.multiple_of(h * pol, rows), rows) for h in (base, other))

    def near_sum(at):
        return jnp.dot(
            picks[side, at, :], near_recv[...].reshape(team * sites, width), preferred_element_type=f32
        )

    with jax.named_scope("nearsum"):
        part_send[...] = near_sum(theirs_at).astype(bf16).reshape(team, pol, width)
        loop(0, team, lambda i: part_copy(turn(i)).start())
    with jax.named_scope("nearsum2"):
        near_acc[...] = near_sum(ours_at)
    with jax.named_scope("learn2"):
        learn(other)
    with jax.named_scope("fullwait"):
        bulk(FULL, full_recv.at[pl.ds(0, n - 1)]).wait_recv()
    with jax.named_scope("fullsum"):

        def unpacked(k):
            packed = full_recv[k * team : (k + 1) * team]
            return jnp.concatenate([packed, swap(packed)], axis=1).reshape(team * sites, width)

        total = jnp.dot(picks[0], unpacked(0), preferred_element_type=f32) + jnp.dot(
            picks[1], unpacked(1), preferred_element_type=f32
        )
        loss = terms(total, *spread_of(policy_terms, every, width // LANES))
        split = loss.reshape(n, 2, pol // 2, width)
        mask = lax.broadcasted_iota(jnp.int32, (n, pol // 2, width), 2) < width // 2
        full_losses[...] = jnp.where(mask, split[:, 0], swap(split[:, 1])).astype(bf16)
        others(lambda d: full_policy_copy(d).start())
        full_policy[me] = full_losses[me]
        loss = loss.astype(bf16)
        gross = jnp.dot(marks[0], loss[0:rows], preferred_element_type=f32) + jnp.dot(
            marks[1], loss[rows : 2 * rows], preferred_element_type=f32
        )
        for o in range(n):
            program_send[o, 1] = gross[o * prog : (o + 1) * prog, :]

    def close(i):
        q = turn(i)
        part_copy(q).wait_recv()
        at = rows_of(base + q, pol)
        gross = near_acc[rows_of(q, pol), :] + part_recv[q].astype(f32)
        loss = terms(gross, *spread_of(policy_terms, at, width // LANES)).astype(bf16)
        near_losses[rows_of(q, pol), :] = loss

        @pl.when(q != seat)
        def _():
            near_policy_copy(q).start()

        @pl.when(q == seat)
        def _():
            policy_out[:, columns_of(2 * seat)] = loss

    with jax.named_scope("close"):
        loop(0, team, close)
    with jax.named_scope("progsend"):
        near_gross = jnp.dot(marks[side], near_losses[...], preferred_element_type=f32)
        for o in range(n):
            program_send[o, 0] = near_gross[o * prog : (o + 1) * prog, :]
        others(lambda d: program_copy(d).start())
        program_recv[me] = program_send[me]
    with jax.named_scope("fpolwait"):
        bulk(FULL_POLICY, full_policy.at[pl.ds(0, n - 1)]).wait_recv()
        low = lax.broadcasted_iota(jnp.int32, (pol // 2, width), 1) < width // 2
        for g in range(team):
            left, right = full_policy[g].astype(f32), full_policy[team + g].astype(f32)
            at = slice((2 * g + 1) * width, (2 * g + 2) * width)
            policy_out[: pol // 2, at] = jnp.where(low, left, swap(right)).astype(bf16)
            policy_out[pol // 2 :, at] = jnp.where(low, swap(left), right).astype(bf16)
    with jax.named_scope("sent"):
        bulk(META, meta.at[pl.ds(0, n - 1)]).wait_send()
        bulk(NEAR, near_send.at[pl.ds(0, team - 1)]).wait_send()
        bulk(FULL, full_send.at[pl.ds(0, n - 1)]).wait_send()
        bulk(PART, part_send).wait_send()
        bulk(NEAR_POLICY, near_losses.at[pl.ds(0, rows - pol), :]).wait_send()
        bulk(FULL_POLICY, full_losses.at[pl.ds(0, n - 1)]).wait_send()
        bulk(PROGRAM, program_send.at[pl.ds(0, n - 1)]).wait_send()
    with jax.named_scope("npolwait"):
        bulk(NEAR_POLICY, near_losses.at[pl.ds(0, rows - pol), :]).wait_recv()
    with jax.named_scope("progwait"):
        bulk(PROGRAM, program_recv.at[pl.ds(0, n - 1)]).wait_recv()
    with jax.named_scope("tail"):
        spread = spread_of(program_terms, every, width // LANES)
        low = lax.broadcasted_iota(jnp.int32, (prog, width), 1) < width // 2
        for g in range(team):
            near = program_recv[g, 0] + program_recv[team + g, 0]
            full = jnp.where(low, program_recv[g, 1], swap(program_recv[team + g, 1]))
            at = 2 * g * width
            program_out[:, at : at + width] = terms(near, *spread)
            program_out[:, at + width : at + 2 * width] = terms(full, *spread)


def exchange(
    ground_up,
    item_site,
    item_profile,
    site_owner,
    site_slot,
    site_profile,
    policy_owner,
    policy_slot,
    policy_profile,
    program_profile,
    term_table,
):
    n = lax.axis_size("own")
    items, cols = ground_up.shape
    sites = site_profile.shape[0]
    pol = policy_profile.shape[0]
    prog = program_profile.shape[0]
    width = cols // n
    team = n // 2

    def row(v):
        return v.reshape(-1, min(v.size, LANES))

    inputs = [
        row(v)
        for v in (
            item_site,
            item_profile,
            site_owner,
            site_slot,
            site_profile,
            policy_owner,
            policy_slot,
            policy_profile,
            program_profile,
        )
    ] + [term_table.transpose(1, 0, 2)]
    vmemspec = pl.BlockSpec(memory_space=pltpu.VMEM)
    anyspec = pl.BlockSpec(memory_space=pl.ANY)
    dma = pltpu.SemaphoreType.DMA
    return pl.pallas_call(
        functools.partial(kernel, n, pol, prog),
        out_shape=(
            pltpu.VMEM((pol, cols), bf16),
            pltpu.VMEM((prog, cols), f32),
        ),
        in_specs=[anyspec] * (1 + SMALL),
        out_specs=(vmemspec, vmemspec),
        scratch_shapes=[
            pltpu.VMEM((2 * (items // LANES), LANES), jnp.int32),
            pltpu.VMEM((3, sites), jnp.int32),
            pltpu.VMEM((3, pol), jnp.int32),
            pltpu.VMEM((1, prog), jnp.int32),
            pltpu.VMEM(inputs[-1].shape, f32),
            pltpu.VMEM((team, items, 2 * width), bf16),
            pltpu.VMEM((8, LANES), jnp.int32),
            pltpu.VMEM((LANES, LANES), f32),
            pltpu.VMEM((3, items, LANES), f32),
            pltpu.VMEM((3, sites, LANES), f32),
            pltpu.VMEM((3, n * pol, LANES), f32),
            pltpu.VMEM((3, prog, LANES), f32),
            pltpu.VMEM((sites, items), bf16),
            pltpu.VMEM((n, 2, LANES), jnp.int32),
            pltpu.VMEM((team, sites, width), bf16),
            pltpu.VMEM((team, sites, width), bf16),
            pltpu.VMEM((n, sites // 2, width), bf16),
            pltpu.VMEM((n, sites // 2, width), bf16),
            pltpu.VMEM((team, pol, width), bf16),
            pltpu.VMEM((team, pol, width), bf16),
            pltpu.VMEM((team * pol, width), f32),
            pltpu.VMEM((team * pol, width), bf16),
            pltpu.VMEM((n, pol // 2, width), bf16),
            pltpu.VMEM((n, pol // 2, width), bf16),
            pltpu.VMEM((n, 2, prog, width), f32),
            pltpu.VMEM((n, 2, prog, width), f32),
            pltpu.VMEM((2, n * prog, team * pol), bf16),
            pltpu.VMEM((2, n * pol, team * sites), bf16),
            dma((5,)),
            dma((team,)),
            dma((team,)),
            dma((7,)),
            dma((7,)),
        ],
        compiler_params=pltpu.CompilerParams(collective_id=0, has_side_effects=True),
        name="loss_terms",
    )(ground_up, *inputs)


def apply_terms(gross_loss, terms_table, tier_index, profile):
    profile_iota = jnp.arange(terms_table.shape[2], dtype=jnp.int32)
    picker = profile[:, None] == profile_iota[None, :]
    deduct = jnp.sum(jnp.where(picker, terms_table[tier_index, 0][None, :], 0.0), axis=1)[:, None]
    ceiling = jnp.sum(jnp.where(picker, terms_table[tier_index, 1][None, :], 0.0), axis=1)[:, None]
    portion = jnp.sum(jnp.where(picker, terms_table[tier_index, 2][None, :], 0.0), axis=1)[:, None]
    return portion * jnp.minimum(jnp.maximum(gross_loss - deduct, 0.0), ceiling)


def pack_rows(values, target_dev, inner_slot, owners, capacity):
    member = (target_dev[:, None] == jnp.arange(owners, dtype=jnp.int32)[None, :]).astype(jnp.int32)
    before = jnp.cumsum(member, axis=0) - member
    position = jnp.sum(before * member, axis=1)
    target = target_dev * capacity + position
    placer = jnp.arange(owners * capacity, dtype=jnp.int32)[:, None] == target[None, :]
    packed = jnp.dot(
        placer.astype(jnp.bfloat16), values, preferred_element_type=jnp.float32
    ).astype(jnp.bfloat16)
    labels = jnp.sum(jnp.where(placer, (inner_slot + 1)[None, :], 0), axis=1) - 1
    return (
        packed.reshape(owners, capacity, values.shape[1]),
        labels.astype(jnp.bfloat16).reshape(owners, capacity),
    )


def sum_rows(received, labels, slot_count):
    flattened = received.reshape(-1, received.shape[2])
    slot_marks = labels.reshape(-1).astype(jnp.int32)
    picker = (jnp.arange(slot_count, dtype=jnp.int32)[:, None] == slot_marks[None, :]).astype(
        jnp.bfloat16
    )
    return jnp.dot(picker, flattened, preferred_element_type=jnp.float32)


def shards(
    ground_up,
    item_site,
    item_profile,
    site_owner,
    site_slot,
    site_profile,
    policy_owner,
    policy_slot,
    policy_profile,
    program_profile,
    term_table,
):
    owners = lax.axis_size("own")
    covered = apply_terms(ground_up.astype(jnp.float32), term_table, 0, item_profile).astype(
        jnp.bfloat16
    )
    site_total = site_profile.shape[0]
    grouping = (jnp.arange(site_total, dtype=jnp.int32)[:, None] == item_site[None, :]).astype(
        jnp.bfloat16
    )
    site_gross = jnp.dot(grouping, covered, preferred_element_type=jnp.float32)
    site_net = apply_terms(site_gross, term_table, 1, site_profile).astype(jnp.bfloat16)
    capacity = 2 * site_total // owners
    packed, labels = pack_rows(site_net, site_owner[:, 0], site_slot, owners, capacity)
    arrived, arrived_labels = (
        lax.all_to_all(packed, "own", split_axis=0, concat_axis=0, tiled=True),
        lax.all_to_all(labels, "own", split_axis=0, concat_axis=0, tiled=True),
    )
    policy_total = policy_profile.shape[0]
    policy_gross = sum_rows(arrived, arrived_labels, policy_total)
    policy_loss = apply_terms(policy_gross, term_table, 2, policy_profile).astype(jnp.bfloat16)
    program_total = program_profile.shape[0]
    program_capacity = 3 * policy_total // owners
    sent_rows, sent_labels = pack_rows(
        policy_loss, policy_owner[:, 0], policy_slot, owners, program_capacity
    )
    got_rows, got_labels = (
        lax.all_to_all(sent_rows, "own", split_axis=0, concat_axis=0, tiled=True),
        lax.all_to_all(sent_labels, "own", split_axis=0, concat_axis=0, tiled=True),
    )
    program_gross = sum_rows(got_rows, got_labels, program_total)
    program_loss = apply_terms(program_gross, term_table, 3, program_profile)
    return (policy_loss, program_loss)


def solution(mesh):
    placed = (
        P("own", "ev"),
        P("own"),
        P("own"),
        P("own", None),
        P("own"),
        P("own"),
        P("own", None),
        P("own"),
        P("own"),
        P("own"),
        P(),
    )

    def body(ground_up, item_site, item_profile, *rest):
        n = lax.axis_size("own")
        items, cols = ground_up.shape
        sites, pol = rest[2].shape[0], rest[5].shape[0]
        prog = rest[6].shape[0]
        fits = cols % (n * LANES) == 0 and items % LANES == 0 and sites == LANES
        fits = fits and 2 * pol <= LANES and pol % 16 == 0 and prog <= 8
        fits = fits and n % 4 == 0 and n & (n - 1) == 0 and 3 * n <= LANES and 3 * items <= LANES * (LANES - 6)
        return (exchange if fits else shards)(ground_up, item_site, item_profile, *rest)

    return jax.shard_map(
        body,
        mesh=mesh,
        in_specs=placed,
        out_specs=(P("own", "ev"), P("own", "ev")),
        check_vma=False,
    )
```

```python
import functools

import jax
import jax.numpy as jnp
from jax import lax
from jax.experimental import pallas as pl
from jax.experimental.pallas import tpu as pltpu
from jax.sharding import PartitionSpec as P

LANES = 128
SMALL = 10
f32 = jnp.float32
bf16 = jnp.bfloat16


def terms(x, deduct, ceiling, portion):
    return portion * jnp.minimum(jnp.maximum(x - deduct, 0.0), ceiling)


def mixed(a, b, n):
    d, bit = 0, 1
    while bit < n:
        d = d + bit * lax.rem(lax.div(a, bit) + lax.div(b, bit), 2)
        bit *= 2
    return d


def kernel(
    n,
    pol,
    prog,
    ground,
    *refs,
):
    small_in, refs = refs[:SMALL], refs[SMALL:]
    policy_out, program_out = refs[:2]
    (
        item_rows,
        site_rows,
        policy_rows,
        program_row,
        table,
        chunks,
        ids,
        square,
        item_terms,
        site_terms,
        policy_terms,
        program_terms,
        grouping,
        meta,
        near_send,
        near_recv,
        full_send,
        full_recv,
        part_send,
        part_recv,
        near_acc,
        near_losses,
        full_losses,
        full_policy,
        program_send,
        program_recv,
        marks,
        picks,
        small_sem,
        load_sem,
        part_rs,
        sends,
        recvs,
    ) = refs[2:]
    me = lax.axis_index("own")
    team = n // 2
    side = lax.div(me, team)
    seat = lax.rem(me, team)
    base = side * team
    other = (1 - side) * team
    mate = other + seat
    items = ground.shape[0]
    blocks = items // LANES
    sites = near_send.shape[1]
    width = near_send.shape[2]
    wide = 2 * width
    rows = team * pol
    META, NEAR, FULL, PART, NEAR_POLICY, FULL_POLICY, PROGRAM = range(7)

    def turn(i):
        half = team // 2
        late = lax.div(i, half)
        return mixed(seat, (1 - late) * (i + half) + late * lax.rem(i + 1, half), team)

    barrier = pltpu.get_barrier_semaphore()

    def greet(k, c):
        pl.semaphore_signal(barrier, inc=1, device_id={"own": lax.rem(me + k, n)})
        return c

    homes = (
        [item_rows.at[pl.ds(i * blocks, blocks), :] for i in range(2)]
        + [site_rows.at[pl.ds(i, 1), :] for i in range(3)]
        + [policy_rows.at[pl.ds(i, 1), :] for i in range(3)]
        + [program_row, table]
    )
    for i, (src, dst) in enumerate(zip(small_in, homes)):
        pltpu.make_async_copy(src, dst, small_sem.at[(0, 0, 1, 1, 1, 2, 2, 2, 3, 4)[i]]).start()

    lax.fori_loop(1, n, greet, 0)

    def load(i):
        return pltpu.make_async_copy(
            ground.at[:, pl.ds(pl.multiple_of(turn(i) * wide, wide), wide)],
            chunks.at[i],
            load_sem.at[i],
        )

    def start_load(i, c):
        load(i).start()
        return c

    lax.fori_loop(0, team, start_load, 0)
    with jax.named_scope("small"):
        for i, whole in enumerate((item_rows, site_rows, policy_rows, program_row, table)):
            pltpu.make_async_copy(whole, whole, small_sem.at[i]).wait()

    square[...] = jnp.zeros_like(square)
    for t in range(3):
        square[4 * t : 4 * t + 4, :] = table[t]
    columns = square[...].T
    rows_iota = lax.broadcasted_iota(jnp.int32, (LANES, LANES), 0)

    def look(profile_row, level):
        pick = rows_iota == profile_row
        return [
            jnp.sum(
                jnp.where(pick, columns[:, 4 * t + level : 4 * t + level + 1], 0.0),
                axis=0,
                keepdims=True,
            )
            for t in range(3)
        ]

    with jax.named_scope("prep"):
        ids[...] = jnp.zeros_like(ids)
        ids[0:1, 0:pol] = policy_rows[2:3, :]
        ids[0:1, pol : 2 * pol] = policy_rows[0:1, :] * prog + policy_rows[1:2, :]
        ids[1:2, 0:prog] = program_row[...]
        meta[me] = jnp.concatenate([site_rows[0:1, :] * pol + site_rows[1:2, :], ids[0:1, :]], axis=0)

        for b in range(blocks):
            grouping[:, b * LANES : (b + 1) * LANES] = (rows_iota == item_rows[b : b + 1, :]).astype(bf16)
            for t, row in enumerate(look(item_rows[blocks + b : blocks + b + 1, :], 0)):
                square[3 * b + t : 3 * b + t + 1, :] = row
        for t, row in enumerate(look(site_rows[2:3, :], 1)):
            square[3 * blocks + t : 3 * blocks + t + 1, :] = row
        for t, row in enumerate(look(ids[1:2, :], 3)):
            square[3 * blocks + 3 + t : 3 * blocks + 4 + t, :] = row
        flipped = square[...].T
        for t in range(3):
            for b in range(blocks):
                item_terms[t, b * LANES : (b + 1) * LANES, :] = jnp.broadcast_to(
                    flipped[:, 3 * b + t : 3 * b + t + 1], (LANES, LANES)
                )
            program_terms[t] = jnp.broadcast_to(
                flipped[0:prog, 3 * blocks + 3 + t : 3 * blocks + 4 + t], (prog, LANES)
            )
            site_terms[t] = jnp.broadcast_to(
                flipped[:, 3 * blocks + t : 3 * blocks + t + 1], (LANES, LANES)
            )

    def remote(kind, src, dst, d):
        return pltpu.make_async_remote_copy(src, dst, sends.at[kind], recvs.at[kind], device_id={"own": d})

    def columns_of(block):
        return pl.ds(pl.multiple_of(block * width, width), width)

    def rows_of(q, count):
        return pl.ds(pl.multiple_of(q * count, count), count)

    def meta_copy(d):
        return remote(META, meta.at[me], meta.at[me], d)

    def near_copy(g):
        return remote(NEAR, near_send.at[g], near_recv.at[seat], base + g)

    def full_copy(d):
        return remote(FULL, full_send.at[d], full_recv.at[me], d)

    chunk = team // 2

    def part_copy(q):
        at = pl.ds(q * chunk, chunk)
        return pltpu.make_async_remote_copy(
            part_send.at[at], part_recv.at[at], sends.at[PART], part_rs.at[q], device_id={"own": mate}
        )

    def near_policy_copy(q):
        return remote(
            NEAR_POLICY, near_losses.at[rows_of(q, pol), :], policy_out.at[:, columns_of(2 * seat)], base + q
        )

    def full_policy_copy(d):
        return remote(FULL_POLICY, full_losses.at[d], full_policy.at[me], d)

    def program_copy(d):
        return remote(PROGRAM, program_send.at[d], program_recv.at[me], d)

    def bulk(kind, ref):
        return remote(kind, ref, ref, me)

    def others(fn):
        def step(k, c):
            fn(mixed(me, n - k, n))
            return c

        lax.fori_loop(1, n, step, 0)

    def loop(start, stop, fn):
        def step(i, c):
            fn(i)
            return c

        lax.fori_loop(start, stop, step, 0)

    def spread_of(refs_terms, at, count):
        return [jnp.concatenate([refs_terms[t, at, :]] * count, axis=1) for t in range(3)]

    every = slice(None)
    low_half = lax.broadcasted_iota(jnp.int32, (sites // 2, width), 1) < width // 2

    def swap(x):
        return pltpu.roll(x, width // 2, x.ndim - 1)

    def site_losses(i):
        load(i).wait()
        g = turn(i)
        covered = terms(chunks[i].astype(f32), *spread_of(item_terms, every, wide // LANES)).astype(bf16)
        gross = jnp.dot(grouping[...], covered, preferred_element_type=f32)
        net = terms(gross, *spread_of(site_terms, every, wide // LANES))
        near = net[:, :width].astype(bf16)
        top, bottom = net[: sites // 2, width:], net[sites // 2 :, width:]
        left = jnp.where(low_half, top, swap(bottom)).astype(bf16)
        right = jnp.where(low_half, swap(top), bottom).astype(bf16)
        ours = jnp.where(side == 0, left, right)
        theirs = jnp.where(side == 0, right, left)
        full_send[other + g] = theirs

        @pl.when(g == seat)
        def _():
            near_recv[seat] = near
            full_recv[me] = ours

        @pl.when(g != seat)
        def _():
            near_send[g] = near
            full_send[base + g] = ours

    lag = team // 2
    inner = lax.rem(lax.div(seat, lag) + side, 2)

    def send_near(i):
        near_copy(turn(i)).start()

    def send_cross(i):
        full_copy(other + turn(i)).start()

    plane, corner = lax.div(me, 4), lax.rem(me, 4)
    hops = plane + lax.div(corner, 2) + lax.rem(corner, 2)
    ahead = lax.clamp(1, 13 - 3 * hops, team - 1)
    with jax.named_scope("first"):
        loop(0, ahead, site_losses)
    with jax.named_scope("bar"):
        pl.semaphore_wait(barrier, n - 1)
    with jax.named_scope("sites"):
        others(lambda d: meta_copy(d).start())

        def send(i):
            send_near(i)
            @pl.when(inner == 1)
            def _():
                send_cross(i)

            @pl.when((inner == 0) & (i >= lag))
            def _():
                send_cross(i - lag)

        def step(i):
            site_losses(i)
            send(i)

        loop(0, ahead, send)
        loop(ahead, team - 1, step)
        site_losses(team - 1)
        loop(lax.select(inner == 1, team - 1, lag - 1), team, send_cross)
        loop(0, team - 1, lambda i: full_copy(base + turn(i)).start())
    with jax.named_scope("metawait"):
        bulk(META, meta.at[pl.ds(0, n - 1)]).wait_recv()

    policy_iota = lax.broadcasted_iota(jnp.int32, (n * pol, sites), 0)
    program_iota = lax.broadcasted_iota(jnp.int32, (n * prog, pol), 0)

    def learn(start):
        for o in range(team):
            for t, row in enumerate(look(meta[start + o][1:2, :], 2)):
                square[3 * o + t : 3 * o + t + 1, :] = row
        turned = square[...].T
        for o in range(team):
            for t in range(3):
                lane = 3 * o + t
                policy_terms[t, rows_of(start + o, pol), :] = jnp.broadcast_to(
                    turned[0:pol, lane : lane + 1], (pol, LANES)
                )
        which = lax.div(start, team)
        marks[which] = jnp.concatenate(
            [(program_iota == meta[start + o][1:2, pol : 2 * pol]).astype(bf16) for o in range(team)], axis=1
        )
        for o in range(team):
            picks[which, :, o * sites : (o + 1) * sites] = (policy_iota == meta[start + o][0:1, :]).astype(bf16)

    with jax.named_scope("learn"):
        learn(base)
    with jax.named_scope("nearwait"):
        bulk(NEAR, near_recv.at[pl.ds(0, team - 1)]).wait_recv()
    ours_at, theirs_at = (pl.ds(pl.multiple_of(h * pol, rows), rows) for h in (base, other))

    def near_sum(at):
        return jnp.dot(
            picks[side, at, :], near_recv[...].reshape(team * sites, width), preferred_element_type=f32
        )

    with jax.named_scope("nearsum"):
        part_send[...] = near_sum(theirs_at).astype(bf16).reshape(team, pol, width)
        loop(0, 2, lambda i: part_copy(lax.rem(i + lax.div(seat, chunk), 2)).start())
    with jax.named_scope("nearsum2"):
        near_acc[...] = near_sum(ours_at)
    with jax.named_scope("learn2"):
        learn(other)
    with jax.named_scope("fullwait"):
        bulk(FULL, full_recv.at[pl.ds(0, n - 1)]).wait_recv()
    with jax.named_scope("fullsum"):

        def unpacked(k):
            packed = full_recv[k * team : (k + 1) * team]
            return jnp.concatenate([packed, swap(packed)], axis=1).reshape(team * sites, width)

        total = jnp.dot(picks[0], unpacked(0), preferred_element_type=f32) + jnp.dot(
            picks[1], unpacked(1), preferred_element_type=f32
        )
        loss = terms(total, *spread_of(policy_terms, every, width // LANES))
        split = loss.reshape(n, 2, pol // 2, width)
        mask = lax.broadcasted_iota(jnp.int32, (n, pol // 2, width), 2) < width // 2
        full_losses[...] = jnp.where(mask, split[:, 0], swap(split[:, 1])).astype(bf16)
        others(lambda d: full_policy_copy(d).start())
        full_policy[me] = full_losses[me]
        loss = loss.astype(bf16)
        gross = jnp.dot(marks[0], loss[0:rows], preferred_element_type=f32) + jnp.dot(
            marks[1], loss[rows : 2 * rows], preferred_element_type=f32
        )
        for o in range(n):
            program_send[o, 1] = gross[o * prog : (o + 1) * prog, :]

    def close(i):
        q = lax.rem(i + lax.div(seat, chunk) * chunk, team)

        @pl.when(lax.rem(i, chunk) == 0)
        def _():
            part_copy(lax.div(q, chunk)).wait_recv()

        at = rows_of(base + q, pol)
        gross = near_acc[rows_of(q, pol), :] + part_recv[q].astype(f32)
        loss = terms(gross, *spread_of(policy_terms, at, width // LANES)).astype(bf16)
        near_losses[rows_of(q, pol), :] = loss

        @pl.when(q != seat)
        def _():
            near_policy_copy(q).start()

        @pl.when(q == seat)
        def _():
            policy_out[:, columns_of(2 * seat)] = loss

    with jax.named_scope("close"):
        loop(0, team, close)
    with jax.named_scope("progsend"):
        near_gross = jnp.dot(marks[side], near_losses[...], preferred_element_type=f32)
        for o in range(n):
            program_send[o, 0] = near_gross[o * prog : (o + 1) * prog, :]
        others(lambda d: program_copy(d).start())
        program_recv[me] = program_send[me]
    with jax.named_scope("fpolwait"):
        bulk(FULL_POLICY, full_policy.at[pl.ds(0, n - 1)]).wait_recv()
        low = lax.broadcasted_iota(jnp.int32, (pol // 2, width), 1) < width // 2
        for g in range(team):
            left, right = full_policy[g].astype(f32), full_policy[team + g].astype(f32)
            at = slice((2 * g + 1) * width, (2 * g + 2) * width)
            policy_out[: pol // 2, at] = jnp.where(low, left, swap(right)).astype(bf16)
            policy_out[pol // 2 :, at] = jnp.where(low, swap(left), right).astype(bf16)
    with jax.named_scope("sent"):
        bulk(META, meta.at[pl.ds(0, n - 1)]).wait_send()
        bulk(NEAR, near_send.at[pl.ds(0, team - 1)]).wait_send()
        bulk(FULL, full_send.at[pl.ds(0, n - 1)]).wait_send()
        bulk(PART, part_send).wait_send()
        bulk(NEAR_POLICY, near_losses.at[pl.ds(0, rows - pol), :]).wait_send()
        bulk(FULL_POLICY, full_losses.at[pl.ds(0, n - 1)]).wait_send()
        bulk(PROGRAM, program_send.at[pl.ds(0, n - 1)]).wait_send()
    with jax.named_scope("npolwait"):
        bulk(NEAR_POLICY, near_losses.at[pl.ds(0, rows - pol), :]).wait_recv()
    with jax.named_scope("progwait"):
        bulk(PROGRAM, program_recv.at[pl.ds(0, n - 1)]).wait_recv()
    with jax.named_scope("tail"):
        spread = spread_of(program_terms, every, width // LANES)
        low = lax.broadcasted_iota(jnp.int32, (prog, width), 1) < width // 2
        for g in range(team):
            near = program_recv[g, 0] + program_recv[team + g, 0]
            full = jnp.where(low, program_recv[g, 1], swap(program_recv[team + g, 1]))
            at = 2 * g * width
            program_out[:, at : at + width] = terms(near, *spread)
            program_out[:, at + width : at + 2 * width] = terms(full, *spread)


def store(policy, program, policy_out, program_out, sems):
    copies = [
        pltpu.make_async_copy(policy, policy_out, sems.at[0]),
        pltpu.make_async_copy(program, program_out, sems.at[1]),
    ]
    for copy in copies:
        copy.start()
    for copy in copies:
        copy.wait()


def exchange(
    ground_up,
    item_site,
    item_profile,
    site_owner,
    site_slot,
    site_profile,
    policy_owner,
    policy_slot,
    policy_profile,
    program_profile,
    term_table,
):
    n = lax.axis_size("own")
    items, cols = ground_up.shape
    sites = site_profile.shape[0]
    pol = policy_profile.shape[0]
    prog = program_profile.shape[0]
    width = cols // n
    team = n // 2

    def row(v):
        return v.reshape(-1, min(v.size, LANES))

    inputs = [
        row(v)
        for v in (
            item_site,
            item_profile,
            site_owner,
            site_slot,
            site_profile,
            policy_owner,
            policy_slot,
            policy_profile,
            program_profile,
        )
    ] + [term_table.transpose(1, 0, 2)]
    vmemspec = pl.BlockSpec(memory_space=pltpu.VMEM)
    anyspec = pl.BlockSpec(memory_space=pl.ANY)
    dma = pltpu.SemaphoreType.DMA
    held = pl.pallas_call(
        functools.partial(kernel, n, pol, prog),
        out_shape=(
            pltpu.VMEM((pol, cols), bf16),
            pltpu.VMEM((prog, cols), f32),
        ),
        in_specs=[anyspec] * (1 + SMALL),
        out_specs=(vmemspec, vmemspec),
        scratch_shapes=[
            pltpu.VMEM((2 * (items // LANES), LANES), jnp.int32),
            pltpu.VMEM((3, sites), jnp.int32),
            pltpu.VMEM((3, pol), jnp.int32),
            pltpu.VMEM((1, prog), jnp.int32),
            pltpu.VMEM(inputs[-1].shape, f32),
            pltpu.VMEM((team, items, 2 * width), bf16),
            pltpu.VMEM((8, LANES), jnp.int32),
            pltpu.VMEM((LANES, LANES), f32),
            pltpu.VMEM((3, items, LANES), f32),
            pltpu.VMEM((3, sites, LANES), f32),
            pltpu.VMEM((3, n * pol, LANES), f32),
            pltpu.VMEM((3, prog, LANES), f32),
            pltpu.VMEM((sites, items), bf16),
            pltpu.VMEM((n, 2, LANES), jnp.int32),
            pltpu.VMEM((team, sites, width), bf16),
            pltpu.VMEM((team, sites, width), bf16),
            pltpu.VMEM((n, sites // 2, width), bf16),
            pltpu.VMEM((n, sites // 2, width), bf16),
            pltpu.VMEM((team, pol, width), bf16),
            pltpu.VMEM((team, pol, width), bf16),
            pltpu.VMEM((team * pol, width), f32),
            pltpu.VMEM((team * pol, width), bf16),
            pltpu.VMEM((n, pol // 2, width), bf16),
            pltpu.VMEM((n, pol // 2, width), bf16),
            pltpu.VMEM((n, 2, prog, width), f32),
            pltpu.VMEM((n, 2, prog, width), f32),
            pltpu.VMEM((2, n * prog, team * pol), bf16),
            pltpu.VMEM((2, n * pol, team * sites), bf16),
            dma((5,)),
            dma((team,)),
            dma((2,)),
            dma((7,)),
            dma((7,)),
        ],
        compiler_params=pltpu.CompilerParams(collective_id=0, has_side_effects=True),
        name="loss_terms",
    )(ground_up, *inputs)
    held = [pltpu.with_memory_space_constraint(v, pltpu.VMEM) for v in held]
    return pl.pallas_call(
        store,
        out_shape=tuple(jax.ShapeDtypeStruct(v.shape, v.dtype) for v in held),
        in_specs=[vmemspec] * 2,
        out_specs=(anyspec, anyspec),
        scratch_shapes=[dma((2,))],
        name="store_losses",
    )(*held)


def apply_terms(gross_loss, terms_table, tier_index, profile):
    profile_iota = jnp.arange(terms_table.shape[2], dtype=jnp.int32)
    picker = profile[:, None] == profile_iota[None, :]
    deduct = jnp.sum(jnp.where(picker, terms_table[tier_index, 0][None, :], 0.0), axis=1)[:, None]
    ceiling = jnp.sum(jnp.where(picker, terms_table[tier_index, 1][None, :], 0.0), axis=1)[:, None]
    portion = jnp.sum(jnp.where(picker, terms_table[tier_index, 2][None, :], 0.0), axis=1)[:, None]
    return portion * jnp.minimum(jnp.maximum(gross_loss - deduct, 0.0), ceiling)


def pack_rows(values, target_dev, inner_slot, owners, capacity):
    member = (target_dev[:, None] == jnp.arange(owners, dtype=jnp.int32)[None, :]).astype(jnp.int32)
    before = jnp.cumsum(member, axis=0) - member
    position = jnp.sum(before * member, axis=1)
    target = target_dev * capacity + position
    placer = jnp.arange(owners * capacity, dtype=jnp.int32)[:, None] == target[None, :]
    packed = jnp.dot(
        placer.astype(jnp.bfloat16), values, preferred_element_type=jnp.float32
    ).astype(jnp.bfloat16)
    labels = jnp.sum(jnp.where(placer, (inner_slot + 1)[None, :], 0), axis=1) - 1
    return (
        packed.reshape(owners, capacity, values.shape[1]),
        labels.astype(jnp.bfloat16).reshape(owners, capacity),
    )


def sum_rows(received, labels, slot_count):
    flattened = received.reshape(-1, received.shape[2])
    slot_marks = labels.reshape(-1).astype(jnp.int32)
    picker = (jnp.arange(slot_count, dtype=jnp.int32)[:, None] == slot_marks[None, :]).astype(
        jnp.bfloat16
    )
    return jnp.dot(picker, flattened, preferred_element_type=jnp.float32)


def shards(
    ground_up,
    item_site,
    item_profile,
    site_owner,
    site_slot,
    site_profile,
    policy_owner,
    policy_slot,
    policy_profile,
    program_profile,
    term_table,
):
    owners = lax.axis_size("own")
    covered = apply_terms(ground_up.astype(jnp.float32), term_table, 0, item_profile).astype(
        jnp.bfloat16
    )
    site_total = site_profile.shape[0]
    grouping = (jnp.arange(site_total, dtype=jnp.int32)[:, None] == item_site[None, :]).astype(
        jnp.bfloat16
    )
    site_gross = jnp.dot(grouping, covered, preferred_element_type=jnp.float32)
    site_net = apply_terms(site_gross, term_table, 1, site_profile).astype(jnp.bfloat16)
    capacity = 2 * site_total // owners
    packed, labels = pack_rows(site_net, site_owner[:, 0], site_slot, owners, capacity)
    arrived, arrived_labels = (
        lax.all_to_all(packed, "own", split_axis=0, concat_axis=0, tiled=True),
        lax.all_to_all(labels, "own", split_axis=0, concat_axis=0, tiled=True),
    )
    policy_total = policy_profile.shape[0]
    policy_gross = sum_rows(arrived, arrived_labels, policy_total)
    policy_loss = apply_terms(policy_gross, term_table, 2, policy_profile).astype(jnp.bfloat16)
    program_total = program_profile.shape[0]
    program_capacity = 3 * policy_total // owners
    sent_rows, sent_labels = pack_rows(
        policy_loss, policy_owner[:, 0], policy_slot, owners, program_capacity
    )
    got_rows, got_labels = (
        lax.all_to_all(sent_rows, "own", split_axis=0, concat_axis=0, tiled=True),
        lax.all_to_all(sent_labels, "own", split_axis=0, concat_axis=0, tiled=True),
    )
    program_gross = sum_rows(got_rows, got_labels, program_total)
    program_loss = apply_terms(program_gross, term_table, 3, program_profile)
    return (policy_loss, program_loss)


def solution(mesh):
    placed = (
        P("own", "ev"),
        P("own"),
        P("own"),
        P("own", None),
        P("own"),
        P("own"),
        P("own", None),
        P("own"),
        P("own"),
        P("own"),
        P(),
    )

    def body(ground_up, item_site, item_profile, *rest):
        n = lax.axis_size("own")
        items, cols = ground_up.shape
        sites, pol = rest[2].shape[0], rest[5].shape[0]
        prog = rest[6].shape[0]
        fits = cols % (n * LANES) == 0 and items % LANES == 0 and sites == LANES
        fits = fits and 2 * pol <= LANES and pol % 16 == 0 and prog <= 8
        fits = fits and n % 4 == 0 and n & (n - 1) == 0 and 3 * n <= LANES and 3 * items <= LANES * (LANES - 6)
        return (exchange if fits else shards)(ground_up, item_site, item_profile, *rest)

    return jax.shard_map(
        body,
        mesh=mesh,
        in_specs=placed,
        out_specs=(P("own", "ev"), P("own", "ev")),
        check_vma=False,
    )
```

```python
import functools

import jax
import jax.numpy as jnp
from jax import lax
from jax.experimental import pallas as pl
from jax.experimental.pallas import tpu as pltpu
from jax.sharding import PartitionSpec as P

LANES = 128
SMALL = 10
f32 = jnp.float32
bf16 = jnp.bfloat16


def terms(x, deduct, ceiling, portion):
    return portion * jnp.minimum(jnp.maximum(x - deduct, 0.0), ceiling)


def mixed(a, b, n):
    d, bit = 0, 1
    while bit < n:
        d = d + bit * lax.rem(lax.div(a, bit) + lax.div(b, bit), 2)
        bit *= 2
    return d


def kernel(
    n,
    pol,
    prog,
    ground,
    *refs,
):
    small_in, refs = refs[:SMALL], refs[SMALL:]
    policy_out, program_out = refs[:2]
    (
        item_rows,
        site_rows,
        policy_rows,
        program_row,
        table,
        chunks,
        ids,
        square,
        item_terms,
        site_terms,
        policy_terms,
        program_terms,
        grouping,
        meta,
        near_send,
        near_recv,
        full_send,
        full_recv,
        part_send,
        part_recv,
        near_acc,
        near_losses,
        full_losses,
        full_policy,
        program_send,
        program_recv,
        marks,
        picks,
        small_sem,
        load_sem,
        part_rs,
        sends,
        recvs,
    ) = refs[2:]
    me = lax.axis_index("own")
    team = n // 2
    side = lax.div(me, team)
    seat = lax.rem(me, team)
    base = side * team
    other = (1 - side) * team
    mate = other + seat
    items = ground.shape[0]
    blocks = items // LANES
    sites = near_send.shape[1]
    width = near_send.shape[2]
    wide = 2 * width
    rows = team * pol
    META, NEAR, FULL, PART, NEAR_POLICY, FULL_POLICY, PROGRAM = range(7)

    def turn(i):
        half = team // 2
        late = lax.div(i, half)
        return mixed(seat, (1 - late) * (i + half) + late * lax.rem(i + 1, half), team)

    barrier = pltpu.get_barrier_semaphore()

    def greet(k, c):
        pl.semaphore_signal(barrier, inc=1, device_id={"own": lax.rem(me + k, n)})
        return c

    homes = (
        [item_rows.at[pl.ds(i * blocks, blocks), :] for i in range(2)]
        + [site_rows.at[pl.ds(i, 1), :] for i in range(3)]
        + [policy_rows.at[pl.ds(i, 1), :] for i in range(3)]
        + [program_row, table]
    )
    for i, (src, dst) in enumerate(zip(small_in, homes)):
        pltpu.make_async_copy(src, dst, small_sem.at[(0, 0, 1, 1, 1, 2, 2, 2, 3, 4)[i]]).start()

    lax.fori_loop(1, n, greet, 0)

    def load(i):
        return pltpu.make_async_copy(
            ground.at[:, pl.ds(pl.multiple_of(turn(i) * wide, wide), wide)],
            chunks.at[i],
            load_sem.at[i],
        )

    def start_load(i, c):
        load(i).start()
        return c

    lax.fori_loop(0, team, start_load, 0)
    with jax.named_scope("small"):
        for i, whole in enumerate((item_rows, site_rows, policy_rows, program_row, table)):
            pltpu.make_async_copy(whole, whole, small_sem.at[i]).wait()

    square[...] = jnp.zeros_like(square)
    for t in range(3):
        square[4 * t : 4 * t + 4, :] = table[t]
    columns = square[...].T
    rows_iota = lax.broadcasted_iota(jnp.int32, (LANES, LANES), 0)

    def look(profile_row, level):
        pick = rows_iota == profile_row
        return [
            jnp.sum(
                jnp.where(pick, columns[:, 4 * t + level : 4 * t + level + 1], 0.0),
                axis=0,
                keepdims=True,
            )
            for t in range(3)
        ]

    with jax.named_scope("prep"):
        for b in range(blocks):
            grouping[:, b * LANES : (b + 1) * LANES] = (rows_iota == item_rows[b : b + 1, :]).astype(bf16)
            for t, row in enumerate(look(item_rows[blocks + b : blocks + b + 1, :], 0)):
                square[3 * b + t : 3 * b + t + 1, :] = row
        for t, row in enumerate(look(site_rows[2:3, :], 1)):
            square[3 * blocks + t : 3 * blocks + t + 1, :] = row
        flipped = square[...].T
        for t in range(3):
            for b in range(blocks):
                item_terms[t, b * LANES : (b + 1) * LANES, :] = jnp.broadcast_to(
                    flipped[:, 3 * b + t : 3 * b + t + 1], (LANES, LANES)
                )
            site_terms[t] = jnp.broadcast_to(
                flipped[:, 3 * blocks + t : 3 * blocks + t + 1], (LANES, LANES)
            )

    def remote(kind, src, dst, d):
        return pltpu.make_async_remote_copy(src, dst, sends.at[kind], recvs.at[kind], device_id={"own": d})

    def columns_of(block):
        return pl.ds(pl.multiple_of(block * width, width), width)

    def rows_of(q, count):
        return pl.ds(pl.multiple_of(q * count, count), count)

    def meta_copy(d):
        return remote(META, meta.at[me], meta.at[me], d)

    def near_copy(g):
        return remote(NEAR, near_send.at[g], near_recv.at[seat], base + g)

    def full_copy(d):
        return remote(FULL, full_send.at[d], full_recv.at[me], d)

    chunk = team // 2

    def part_copy(q):
        at = pl.ds(q * chunk, chunk)
        return pltpu.make_async_remote_copy(
            part_send.at[at], part_recv.at[at], sends.at[PART], part_rs.at[q], device_id={"own": mate}
        )

    def near_policy_copy(q):
        return remote(
            NEAR_POLICY, near_losses.at[rows_of(q, pol), :], policy_out.at[:, columns_of(2 * seat)], base + q
        )

    def full_policy_copy(d):
        return remote(FULL_POLICY, full_losses.at[d], full_policy.at[me], d)

    def program_copy(d):
        return remote(PROGRAM, program_send.at[d], program_recv.at[me], d)

    def bulk(kind, ref):
        return remote(kind, ref, ref, me)

    def others(fn):
        def step(k, c):
            fn(mixed(me, n - k, n))
            return c

        lax.fori_loop(1, n, step, 0)

    def ascending(fn):
        def step(d, c):
            @pl.when(d != me)
            def _():
                fn(d)

            return c

        lax.fori_loop(0, n, step, 0)

    def loop(start, stop, fn):
        def step(i, c):
            fn(i)
            return c

        lax.fori_loop(start, stop, step, 0)

    def spread_of(refs_terms, at, count):
        return [jnp.concatenate([refs_terms[t, at, :]] * count, axis=1) for t in range(3)]

    every = slice(None)
    low_half = lax.broadcasted_iota(jnp.int32, (sites // 2, width), 1) < width // 2

    def swap(x):
        return pltpu.roll(x, width // 2, x.ndim - 1)

    def site_losses(i):
        load(i).wait()
        g = turn(i)
        covered = terms(chunks[i].astype(f32), *spread_of(item_terms, every, wide // LANES)).astype(bf16)
        gross = jnp.dot(grouping[...], covered, preferred_element_type=f32)
        net = terms(gross, *spread_of(site_terms, every, wide // LANES))
        near = net[:, :width].astype(bf16)
        top, bottom = net[: sites // 2, width:], net[sites // 2 :, width:]
        left = jnp.where(low_half, top, swap(bottom)).astype(bf16)
        right = jnp.where(low_half, swap(top), bottom).astype(bf16)
        ours = jnp.where(side == 0, left, right)
        theirs = jnp.where(side == 0, right, left)
        full_send[other + g] = theirs

        @pl.when(g == seat)
        def _():
            near_recv[seat] = near
            full_recv[me] = ours

        @pl.when(g != seat)
        def _():
            near_send[g] = near
            full_send[base + g] = ours

    lag = team // 2
    inner = lax.rem(lax.div(seat, lag) + side, 2)

    def send_near(i):
        near_copy(turn(i)).start()

    def send_cross(i):
        full_copy(other + turn(i)).start()

    plane, corner = lax.div(me, 4), lax.rem(me, 4)
    hops = plane + lax.div(corner, 2) + lax.rem(corner, 2)
    ahead = lax.clamp(1, 13 - 3 * hops, team - 1)
    with jax.named_scope("first"):
        loop(0, ahead, site_losses)
    ids[...] = jnp.zeros_like(ids)
    ids[0:1, 0:pol] = policy_rows[2:3, :]
    ids[0:1, pol : 2 * pol] = policy_rows[0:1, :] * prog + policy_rows[1:2, :]
    ids[1:2, 0:prog] = program_row[...]
    meta[me] = jnp.concatenate([site_rows[0:1, :] * pol + site_rows[1:2, :], ids[0:1, :]], axis=0)

    with jax.named_scope("bar"):
        pl.semaphore_wait(barrier, n - 1)
    with jax.named_scope("sites"):
        loop(1, n, lambda k: meta_copy(lax.rem(me + k, n)).start())

        def send(i):
            send_near(i)
            @pl.when(inner == 1)
            def _():
                send_cross(i)

            @pl.when((inner == 0) & (i >= lag))
            def _():
                send_cross(i - lag)

        def step(i):
            site_losses(i)
            send(i)

        loop(0, ahead, send)
        loop(ahead, team - 1, step)
        site_losses(team - 1)
        loop(lax.select(inner == 1, team - 1, lag - 1), team, send_cross)
        loop(0, team - 1, lambda i: full_copy(base + turn(i)).start())
    with jax.named_scope("metawait"):
        bulk(META, meta.at[pl.ds(0, n - 1)]).wait_recv()

    policy_iota = lax.broadcasted_iota(jnp.int32, (n * pol, sites), 0)
    program_iota = lax.broadcasted_iota(jnp.int32, (n * prog, pol), 0)

    def learn(start):
        for o in range(team):
            for t, row in enumerate(look(meta[start + o][1:2, :], 2)):
                square[3 * o + t : 3 * o + t + 1, :] = row
        turned = square[...].T
        for o in range(team):
            for t in range(3):
                lane = 3 * o + t
                policy_terms[t, rows_of(start + o, pol), :] = jnp.broadcast_to(
                    turned[0:pol, lane : lane + 1], (pol, LANES)
                )
        which = lax.div(start, team)
        marks[which] = jnp.concatenate(
            [(program_iota == meta[start + o][1:2, pol : 2 * pol]).astype(bf16) for o in range(team)], axis=1
        )
        for o in range(team):
            picks[which, :, o * sites : (o + 1) * sites] = (policy_iota == meta[start + o][0:1, :]).astype(bf16)

    with jax.named_scope("learn"):
        learn(base)
    with jax.named_scope("nearwait"):
        bulk(NEAR, near_recv.at[pl.ds(0, team - 1)]).wait_recv()
    ours_at, theirs_at = (pl.ds(pl.multiple_of(h * pol, rows), rows) for h in (base, other))

    def near_sum(at):
        return jnp.dot(
            picks[side, at, :], near_recv[...].reshape(team * sites, width), preferred_element_type=f32
        )

    with jax.named_scope("nearsum"):
        part_send[...] = near_sum(theirs_at).astype(bf16).reshape(team, pol, width)
        loop(0, 2, lambda i: part_copy(lax.rem(i + lax.div(seat, chunk), 2)).start())
    with jax.named_scope("nearsum2"):
        near_acc[...] = near_sum(ours_at)
    with jax.named_scope("learn2"):
        learn(other)
        for t, row in enumerate(look(ids[1:2, :], 3)):
            square[t : t + 1, :] = row
        tilted = square[...].T
        for t in range(3):
            program_terms[t] = jnp.broadcast_to(tilted[0:prog, t : t + 1], (prog, LANES))
    with jax.named_scope("fullwait"):
        bulk(FULL, full_recv.at[pl.ds(0, n - 1)]).wait_recv()
    with jax.named_scope("fullsum"):

        def unpacked(k):
            packed = full_recv[k * team : (k + 1) * team]
            return jnp.concatenate([packed, swap(packed)], axis=1).reshape(team * sites, width)

        total = jnp.dot(picks[0], unpacked(0), preferred_element_type=f32) + jnp.dot(
            picks[1], unpacked(1), preferred_element_type=f32
        )
        loss = terms(total, *spread_of(policy_terms, every, width // LANES))
        split = loss.reshape(n, 2, pol // 2, width)
        mask = lax.broadcasted_iota(jnp.int32, (n, pol // 2, width), 2) < width // 2
        full_losses[...] = jnp.where(mask, split[:, 0], swap(split[:, 1])).astype(bf16)
        core = lax.axis_index("ev")

        @pl.when(core == 0)
        def _():
            ascending(lambda d: full_policy_copy(d).start())

        full_policy[me] = full_losses[me]
        loss = loss.astype(bf16)
        gross = jnp.dot(marks[0], loss[0:rows], preferred_element_type=f32) + jnp.dot(
            marks[1], loss[rows : 2 * rows], preferred_element_type=f32
        )
        for o in range(n):
            program_send[o, 1] = gross[o * prog : (o + 1) * prog, :]

    def close(i):
        q = lax.rem(i + lax.div(seat, chunk) * chunk, team)

        @pl.when(lax.rem(i, chunk) == 0)
        def _():
            part_copy(lax.div(q, chunk)).wait_recv()

        at = rows_of(base + q, pol)
        gross = near_acc[rows_of(q, pol), :] + part_recv[q].astype(f32)
        loss = terms(gross, *spread_of(policy_terms, at, width // LANES)).astype(bf16)
        near_losses[rows_of(q, pol), :] = loss

        @pl.when(q != seat)
        def _():
            near_policy_copy(q).start()

        @pl.when(q == seat)
        def _():
            policy_out[:, columns_of(2 * seat)] = loss

    with jax.named_scope("close"):
        loop(0, team, close)

        @pl.when(core != 0)
        def _():
            ascending(lambda d: full_policy_copy(d).start())

    with jax.named_scope("progsend"):
        near_gross = jnp.dot(marks[side], near_losses[...], preferred_element_type=f32)
        for o in range(n):
            program_send[o, 0] = near_gross[o * prog : (o + 1) * prog, :]
        ascending(lambda d: program_copy(d).start())
        program_recv[me] = program_send[me]
    with jax.named_scope("fpolwait"):
        bulk(FULL_POLICY, full_policy.at[pl.ds(0, n - 1)]).wait_recv()
        low = lax.broadcasted_iota(jnp.int32, (pol // 2, width), 1) < width // 2
        for g in range(team):
            left, right = full_policy[g].astype(f32), full_policy[team + g].astype(f32)
            at = slice((2 * g + 1) * width, (2 * g + 2) * width)
            policy_out[: pol // 2, at] = jnp.where(low, left, swap(right)).astype(bf16)
            policy_out[pol // 2 :, at] = jnp.where(low, swap(left), right).astype(bf16)
    with jax.named_scope("sent"):
        bulk(META, meta.at[pl.ds(0, n - 1)]).wait_send()
        bulk(NEAR, near_send.at[pl.ds(0, team - 1)]).wait_send()
        bulk(FULL, full_send.at[pl.ds(0, n - 1)]).wait_send()
        bulk(PART, part_send).wait_send()
        bulk(NEAR_POLICY, near_losses.at[pl.ds(0, rows - pol), :]).wait_send()
        bulk(FULL_POLICY, full_losses.at[pl.ds(0, n - 1)]).wait_send()
        bulk(PROGRAM, program_send.at[pl.ds(0, n - 1)]).wait_send()
    with jax.named_scope("npolwait"):
        bulk(NEAR_POLICY, near_losses.at[pl.ds(0, rows - pol), :]).wait_recv()
    with jax.named_scope("progwait"):
        bulk(PROGRAM, program_recv.at[pl.ds(0, n - 1)]).wait_recv()
    with jax.named_scope("tail"):
        spread = spread_of(program_terms, every, width // LANES)
        low = lax.broadcasted_iota(jnp.int32, (prog, width), 1) < width // 2
        for g in range(team):
            near = program_recv[g, 0] + program_recv[team + g, 0]
            full = jnp.where(low, program_recv[g, 1], swap(program_recv[team + g, 1]))
            at = 2 * g * width
            program_out[:, at : at + width] = terms(near, *spread)
            program_out[:, at + width : at + 2 * width] = terms(full, *spread)


def store(policy, program, policy_out, program_out, sems):
    copies = [
        pltpu.make_async_copy(policy, policy_out, sems.at[0]),
        pltpu.make_async_copy(program, program_out, sems.at[1]),
    ]
    for copy in copies:
        copy.start()
    for copy in copies:
        copy.wait()


def exchange(
    ground_up,
    item_site,
    item_profile,
    site_owner,
    site_slot,
    site_profile,
    policy_owner,
    policy_slot,
    policy_profile,
    program_profile,
    term_table,
):
    n = lax.axis_size("own")
    items, cols = ground_up.shape
    sites = site_profile.shape[0]
    pol = policy_profile.shape[0]
    prog = program_profile.shape[0]
    width = cols // n
    team = n // 2

    def row(v):
        return v.reshape(-1, min(v.size, LANES))

    inputs = [
        row(v)
        for v in (
            item_site,
            item_profile,
            site_owner,
            site_slot,
            site_profile,
            policy_owner,
            policy_slot,
            policy_profile,
            program_profile,
        )
    ] + [term_table.transpose(1, 0, 2)]
    vmemspec = pl.BlockSpec(memory_space=pltpu.VMEM)
    anyspec = pl.BlockSpec(memory_space=pl.ANY)
    dma = pltpu.SemaphoreType.DMA
    held = pl.pallas_call(
        functools.partial(kernel, n, pol, prog),
        out_shape=(
            pltpu.VMEM((pol, cols), bf16),
            pltpu.VMEM((prog, cols), f32),
        ),
        in_specs=[anyspec] * (1 + SMALL),
        out_specs=(vmemspec, vmemspec),
        scratch_shapes=[
            pltpu.VMEM((2 * (items // LANES), LANES), jnp.int32),
            pltpu.VMEM((3, sites), jnp.int32),
            pltpu.VMEM((3, pol), jnp.int32),
            pltpu.VMEM((1, prog), jnp.int32),
            pltpu.VMEM(inputs[-1].shape, f32),
            pltpu.VMEM((team, items, 2 * width), bf16),
            pltpu.VMEM((8, LANES), jnp.int32),
            pltpu.VMEM((LANES, LANES), f32),
            pltpu.VMEM((3, items, LANES), f32),
            pltpu.VMEM((3, sites, LANES), f32),
            pltpu.VMEM((3, n * pol, LANES), f32),
            pltpu.VMEM((3, prog, LANES), f32),
            pltpu.VMEM((sites, items), bf16),
            pltpu.VMEM((n, 2, LANES), jnp.int32),
            pltpu.VMEM((team, sites, width), bf16),
            pltpu.VMEM((team, sites, width), bf16),
            pltpu.VMEM((n, sites // 2, width), bf16),
            pltpu.VMEM((n, sites // 2, width), bf16),
            pltpu.VMEM((team, pol, width), bf16),
            pltpu.VMEM((team, pol, width), bf16),
            pltpu.VMEM((team * pol, width), f32),
            pltpu.VMEM((team * pol, width), bf16),
            pltpu.VMEM((n, pol // 2, width), bf16),
            pltpu.VMEM((n, pol // 2, width), bf16),
            pltpu.VMEM((n, 2, prog, width), f32),
            pltpu.VMEM((n, 2, prog, width), f32),
            pltpu.VMEM((2, n * prog, team * pol), bf16),
            pltpu.VMEM((2, n * pol, team * sites), bf16),
            dma((5,)),
            dma((team,)),
            dma((2,)),
            dma((7,)),
            dma((7,)),
        ],
        compiler_params=pltpu.CompilerParams(collective_id=0, has_side_effects=True),
        name="loss_terms",
    )(ground_up, *inputs)
    held = [pltpu.with_memory_space_constraint(v, pltpu.VMEM) for v in held]
    return pl.pallas_call(
        store,
        out_shape=tuple(jax.ShapeDtypeStruct(v.shape, v.dtype) for v in held),
        in_specs=[vmemspec] * 2,
        out_specs=(anyspec, anyspec),
        scratch_shapes=[dma((2,))],
        name="store_losses",
    )(*held)


def apply_terms(gross_loss, terms_table, tier_index, profile):
    profile_iota = jnp.arange(terms_table.shape[2], dtype=jnp.int32)
    picker = profile[:, None] == profile_iota[None, :]
    deduct = jnp.sum(jnp.where(picker, terms_table[tier_index, 0][None, :], 0.0), axis=1)[:, None]
    ceiling = jnp.sum(jnp.where(picker, terms_table[tier_index, 1][None, :], 0.0), axis=1)[:, None]
    portion = jnp.sum(jnp.where(picker, terms_table[tier_index, 2][None, :], 0.0), axis=1)[:, None]
    return portion * jnp.minimum(jnp.maximum(gross_loss - deduct, 0.0), ceiling)


def pack_rows(values, target_dev, inner_slot, owners, capacity):
    member = (target_dev[:, None] == jnp.arange(owners, dtype=jnp.int32)[None, :]).astype(jnp.int32)
    before = jnp.cumsum(member, axis=0) - member
    position = jnp.sum(before * member, axis=1)
    target = target_dev * capacity + position
    placer = jnp.arange(owners * capacity, dtype=jnp.int32)[:, None] == target[None, :]
    packed = jnp.dot(
        placer.astype(jnp.bfloat16), values, preferred_element_type=jnp.float32
    ).astype(jnp.bfloat16)
    labels = jnp.sum(jnp.where(placer, (inner_slot + 1)[None, :], 0), axis=1) - 1
    return (
        packed.reshape(owners, capacity, values.shape[1]),
        labels.astype(jnp.bfloat16).reshape(owners, capacity),
    )


def sum_rows(received, labels, slot_count):
    flattened = received.reshape(-1, received.shape[2])
    slot_marks = labels.reshape(-1).astype(jnp.int32)
    picker = (jnp.arange(slot_count, dtype=jnp.int32)[:, None] == slot_marks[None, :]).astype(
        jnp.bfloat16
    )
    return jnp.dot(picker, flattened, preferred_element_type=jnp.float32)


def shards(
    ground_up,
    item_site,
    item_profile,
    site_owner,
    site_slot,
    site_profile,
    policy_owner,
    policy_slot,
    policy_profile,
    program_profile,
    term_table,
):
    owners = lax.axis_size("own")
    covered = apply_terms(ground_up.astype(jnp.float32), term_table, 0, item_profile).astype(
        jnp.bfloat16
    )
    site_total = site_profile.shape[0]
    grouping = (jnp.arange(site_total, dtype=jnp.int32)[:, None] == item_site[None, :]).astype(
        jnp.bfloat16
    )
    site_gross = jnp.dot(grouping, covered, preferred_element_type=jnp.float32)
    site_net = apply_terms(site_gross, term_table, 1, site_profile).astype(jnp.bfloat16)
    capacity = 2 * site_total // owners
    packed, labels = pack_rows(site_net, site_owner[:, 0], site_slot, owners, capacity)
    arrived, arrived_labels = (
        lax.all_to_all(packed, "own", split_axis=0, concat_axis=0, tiled=True),
        lax.all_to_all(labels, "own", split_axis=0, concat_axis=0, tiled=True),
    )
    policy_total = policy_profile.shape[0]
    policy_gross = sum_rows(arrived, arrived_labels, policy_total)
    policy_loss = apply_terms(policy_gross, term_table, 2, policy_profile).astype(jnp.bfloat16)
    program_total = program_profile.shape[0]
    program_capacity = 3 * policy_total // owners
    sent_rows, sent_labels = pack_rows(
        policy_loss, policy_owner[:, 0], policy_slot, owners, program_capacity
    )
    got_rows, got_labels = (
        lax.all_to_all(sent_rows, "own", split_axis=0, concat_axis=0, tiled=True),
        lax.all_to_all(sent_labels, "own", split_axis=0, concat_axis=0, tiled=True),
    )
    program_gross = sum_rows(got_rows, got_labels, program_total)
    program_loss = apply_terms(program_gross, term_table, 3, program_profile)
    return (policy_loss, program_loss)


def solution(mesh):
    placed = (
        P("own", "ev"),
        P("own"),
        P("own"),
        P("own", None),
        P("own"),
        P("own"),
        P("own", None),
        P("own"),
        P("own"),
        P("own"),
        P(),
    )

    def body(ground_up, item_site, item_profile, *rest):
        n = lax.axis_size("own")
        items, cols = ground_up.shape
        sites, pol = rest[2].shape[0], rest[5].shape[0]
        prog = rest[6].shape[0]
        fits = cols % (n * LANES) == 0 and items % LANES == 0 and sites == LANES
        fits = fits and 2 * pol <= LANES and pol % 16 == 0 and prog <= 8
        fits = fits and n % 4 == 0 and n & (n - 1) == 0 and 3 * n <= LANES and 3 * items <= LANES * (LANES - 6)
        return (exchange if fits else shards)(ground_up, item_site, item_profile, *rest)

    return jax.shard_map(
        body,
        mesh=mesh,
        in_specs=placed,
        out_specs=(P("own", "ev"), P("own", "ev")),
        check_vma=False,
    )
```

```python
import functools

import jax
import jax.numpy as jnp
from jax import lax
from jax.experimental import pallas as pl
from jax.experimental.pallas import tpu as pltpu
from jax.sharding import PartitionSpec as P

LANES = 128
SMALL = 10
f32 = jnp.float32
bf16 = jnp.bfloat16


def terms(x, deduct, ceiling, portion):
    return portion * jnp.minimum(jnp.maximum(x - deduct, 0.0), ceiling)


def mixed(a, b, n):
    d, bit = 0, 1
    while bit < n:
        d = d + bit * lax.rem(lax.div(a, bit) + lax.div(b, bit), 2)
        bit *= 2
    return d


def kernel(
    n,
    pol,
    prog,
    ground,
    *refs,
):
    small_in, refs = refs[:SMALL], refs[SMALL:]
    policy_out, program_out = refs[:2]
    (
        item_rows,
        site_rows,
        policy_rows,
        program_row,
        table,
        chunks,
        ids,
        square,
        item_terms,
        site_terms,
        policy_terms,
        program_terms,
        grouping,
        meta,
        near_send,
        near_recv,
        full_send,
        full_recv,
        part_send,
        part_recv,
        near_acc,
        near_losses,
        full_losses,
        full_policy,
        program_send,
        program_recv,
        marks,
        picks,
        small_sem,
        load_sem,
        part_rs,
        sends,
        recvs,
    ) = refs[2:]
    me = lax.axis_index("own")
    team = n // 2
    side = lax.div(me, team)
    seat = lax.rem(me, team)
    base = side * team
    other = (1 - side) * team
    mate = other + seat
    items = ground.shape[0]
    blocks = items // LANES
    sites = near_send.shape[1]
    width = near_send.shape[2]
    wide = 2 * width
    rows = team * pol
    META, NEAR, FULL, PART, NEAR_POLICY, FULL_POLICY, PROGRAM = range(7)

    def turn(i):
        half = team // 2
        late = lax.div(i, half)
        return mixed(seat, (1 - late) * (i + half) + late * lax.rem(i + 1, half), team)

    barrier = pltpu.get_barrier_semaphore()

    def greet(k, c):
        pl.semaphore_signal(barrier, inc=1, device_id={"own": lax.rem(me + k, n)})
        return c

    homes = (
        [item_rows.at[pl.ds(i * blocks, blocks), :] for i in range(2)]
        + [site_rows.at[pl.ds(i, 1), :] for i in range(3)]
        + [policy_rows.at[pl.ds(i, 1), :] for i in range(3)]
        + [program_row, table]
    )
    for i, (src, dst) in enumerate(zip(small_in, homes)):
        pltpu.make_async_copy(src, dst, small_sem.at[(0, 0, 1, 1, 1, 2, 2, 2, 3, 4)[i]]).start()

    lax.fori_loop(1, n, greet, 0)

    def load(i):
        return pltpu.make_async_copy(
            ground.at[:, pl.ds(pl.multiple_of(turn(i) * wide, wide), wide)],
            chunks.at[i],
            load_sem.at[i],
        )

    def start_load(i, c):
        load(i).start()
        return c

    lax.fori_loop(0, team, start_load, 0)
    with jax.named_scope("small"):
        for i, whole in enumerate((item_rows, site_rows, policy_rows, program_row, table)):
            pltpu.make_async_copy(whole, whole, small_sem.at[i]).wait()

    square[...] = jnp.zeros_like(square)
    for t in range(3):
        square[4 * t : 4 * t + 4, :] = table[t]
    columns = square[...].T
    rows_iota = lax.broadcasted_iota(jnp.int32, (LANES, LANES), 0)

    def look(profile_row, level):
        pick = rows_iota == profile_row
        return [
            jnp.sum(
                jnp.where(pick, columns[:, 4 * t + level : 4 * t + level + 1], 0.0),
                axis=0,
                keepdims=True,
            )
            for t in range(3)
        ]

    with jax.named_scope("prep"):
        for b in range(blocks):
            grouping[:, b * LANES : (b + 1) * LANES] = (rows_iota == item_rows[b : b + 1, :]).astype(bf16)
            for t, row in enumerate(look(item_rows[blocks + b : blocks + b + 1, :], 0)):
                square[3 * b + t : 3 * b + t + 1, :] = row
        for t, row in enumerate(look(site_rows[2:3, :], 1)):
            square[3 * blocks + t : 3 * blocks + t + 1, :] = row
        flipped = square[...].T
        for t in range(3):
            for b in range(blocks):
                item_terms[t, b * LANES : (b + 1) * LANES, :] = jnp.broadcast_to(
                    flipped[:, 3 * b + t : 3 * b + t + 1], (LANES, LANES)
                )
            site_terms[t] = jnp.broadcast_to(
                flipped[:, 3 * blocks + t : 3 * blocks + t + 1], (LANES, LANES)
            )

    def remote(kind, src, dst, d):
        return pltpu.make_async_remote_copy(src, dst, sends.at[kind], recvs.at[kind], device_id={"own": d})

    def columns_of(block):
        return pl.ds(pl.multiple_of(block * width, width), width)

    def rows_of(q, count):
        return pl.ds(pl.multiple_of(q * count, count), count)

    def meta_copy(d):
        return remote(META, meta.at[me], meta.at[me], d)

    def near_copy(g):
        return remote(NEAR, near_send.at[g], near_recv.at[seat], base + g)

    def full_copy(d):
        return remote(FULL, full_send.at[d], full_recv.at[me], d)

    chunk = team // 2

    def part_copy(q):
        at = pl.ds(q * chunk, chunk)
        return pltpu.make_async_remote_copy(
            part_send.at[at], part_recv.at[at], sends.at[PART], part_rs.at[q], device_id={"own": mate}
        )

    def near_policy_copy(q):
        return remote(
            NEAR_POLICY, near_losses.at[rows_of(q, pol), :], policy_out.at[:, columns_of(2 * seat)], base + q
        )

    def full_policy_copy(d):
        return remote(FULL_POLICY, full_losses.at[d], full_policy.at[me], d)

    def program_copy(d):
        return remote(PROGRAM, program_send.at[d], program_recv.at[me], d)

    def bulk(kind, ref):
        return remote(kind, ref, ref, me)

    def others(fn):
        def step(k, c):
            fn(mixed(me, n - k, n))
            return c

        lax.fori_loop(1, n, step, 0)

    def ascending(fn):
        def step(d, c):
            @pl.when(d != me)
            def _():
                fn(d)

            return c

        lax.fori_loop(0, n, step, 0)

    def loop(start, stop, fn):
        def step(i, c):
            fn(i)
            return c

        lax.fori_loop(start, stop, step, 0)

    def spread_of(refs_terms, at, count):
        return [jnp.concatenate([refs_terms[t, at, :]] * count, axis=1) for t in range(3)]

    every = slice(None)
    low_half = lax.broadcasted_iota(jnp.int32, (sites // 2, width), 1) < width // 2

    def swap(x):
        return pltpu.roll(x, width // 2, x.ndim - 1)

    def site_losses(i):
        load(i).wait()
        g = turn(i)
        covered = terms(chunks[i].astype(f32), *spread_of(item_terms, every, wide // LANES)).astype(bf16)
        gross = jnp.dot(grouping[...], covered, preferred_element_type=f32)
        net = terms(gross, *spread_of(site_terms, every, wide // LANES))
        near = net[:, :width].astype(bf16)
        top, bottom = net[: sites // 2, width:], net[sites // 2 :, width:]
        left = jnp.where(low_half, top, swap(bottom)).astype(bf16)
        right = jnp.where(low_half, swap(top), bottom).astype(bf16)
        ours = jnp.where(side == 0, left, right)
        theirs = jnp.where(side == 0, right, left)
        full_send[other + g] = theirs

        @pl.when(g == seat)
        def _():
            near_recv[seat] = near
            full_recv[me] = ours

        @pl.when(g != seat)
        def _():
            near_send[g] = near
            full_send[base + g] = ours

    lag = team // 2 + 1
    inner = lax.rem(lax.div(seat, lag) + side, 2)

    def send_near(i):
        near_copy(turn(i)).start()

    def send_cross(i):
        full_copy(other + turn(i)).start()

    plane, corner = lax.div(me, 4), lax.rem(me, 4)
    hops = plane + lax.div(corner, 2) + lax.rem(corner, 2)
    ahead = lax.clamp(1, 13 - 3 * hops, team - 1)
    with jax.named_scope("first"):
        loop(0, ahead, site_losses)
    ids[...] = jnp.zeros_like(ids)
    ids[0:1, 0:pol] = policy_rows[2:3, :]
    ids[0:1, pol : 2 * pol] = policy_rows[0:1, :] * prog + policy_rows[1:2, :]
    ids[1:2, 0:prog] = program_row[...]
    meta[me] = jnp.concatenate([site_rows[0:1, :] * pol + site_rows[1:2, :], ids[0:1, :]], axis=0)

    with jax.named_scope("bar"):
        pl.semaphore_wait(barrier, n - 1)
    with jax.named_scope("sites"):
        loop(1, n, lambda k: meta_copy(lax.rem(me + k, n)).start())

        def send(i):
            send_near(i)
            @pl.when(inner == 1)
            def _():
                send_cross(i)

            @pl.when((inner == 0) & (i >= lag))
            def _():
                send_cross(i - lag)

        def step(i):
            site_losses(i)
            send(i)

        loop(0, ahead, send)
        loop(ahead, team - 1, step)
        site_losses(team - 1)
        loop(lax.select(inner == 1, team - 1, team - 1 - lag), team, send_cross)
        loop(0, team - 1, lambda i: full_copy(base + turn(i)).start())
    with jax.named_scope("metawait"):
        bulk(META, meta.at[pl.ds(0, n - 1)]).wait_recv()

    policy_iota = lax.broadcasted_iota(jnp.int32, (n * pol, sites), 0)
    program_iota = lax.broadcasted_iota(jnp.int32, (n * prog, pol), 0)

    def learn(start):
        for o in range(team):
            for t, row in enumerate(look(meta[start + o][1:2, :], 2)):
                square[3 * o + t : 3 * o + t + 1, :] = row
        turned = square[...].T
        for o in range(team):
            for t in range(3):
                lane = 3 * o + t
                policy_terms[t, rows_of(start + o, pol), :] = jnp.broadcast_to(
                    turned[0:pol, lane : lane + 1], (pol, LANES)
                )
        which = lax.div(start, team)
        marks[which] = jnp.concatenate(
            [(program_iota == meta[start + o][1:2, pol : 2 * pol]).astype(bf16) for o in range(team)], axis=1
        )
        for o in range(team):
            picks[which, :, o * sites : (o + 1) * sites] = (policy_iota == meta[start + o][0:1, :]).astype(bf16)

    with jax.named_scope("learn"):
        learn(base)
    with jax.named_scope("nearwait"):
        bulk(NEAR, near_recv.at[pl.ds(0, team - 1)]).wait_recv()
    ours_at, theirs_at = (pl.ds(pl.multiple_of(h * pol, rows), rows) for h in (base, other))

    def near_sum(at):
        return jnp.dot(
            picks[side, at, :], near_recv[...].reshape(team * sites, width), preferred_element_type=f32
        )

    with jax.named_scope("nearsum"):
        part_send[...] = near_sum(theirs_at).astype(bf16).reshape(team, pol, width)
        loop(0, 2, lambda i: part_copy(lax.rem(i + lax.div(seat, chunk), 2)).start())
    with jax.named_scope("nearsum2"):
        near_acc[...] = near_sum(ours_at)
    with jax.named_scope("learn2"):
        learn(other)
        for t, row in enumerate(look(ids[1:2, :], 3)):
            square[t : t + 1, :] = row
        tilted = square[...].T
        for t in range(3):
            program_terms[t] = jnp.broadcast_to(tilted[0:prog, t : t + 1], (prog, LANES))
    with jax.named_scope("fullwait"):
        bulk(FULL, full_recv.at[pl.ds(0, n - 1)]).wait_recv()
    with jax.named_scope("fullsum"):

        def unpacked(k):
            packed = full_recv[k * team : (k + 1) * team]
            return jnp.concatenate([packed, swap(packed)], axis=1).reshape(team * sites, width)

        total = jnp.dot(picks[0], unpacked(0), preferred_element_type=f32) + jnp.dot(
            picks[1], unpacked(1), preferred_element_type=f32
        )
        loss = terms(total, *spread_of(policy_terms, every, width // LANES))
        split = loss.reshape(n, 2, pol // 2, width)
        mask = lax.broadcasted_iota(jnp.int32, (n, pol // 2, width), 2) < width // 2
        full_losses[...] = jnp.where(mask, split[:, 0], swap(split[:, 1])).astype(bf16)
        core = lax.axis_index("ev")

        @pl.when(core == 0)
        def _():
            ascending(lambda d: full_policy_copy(d).start())

        full_policy[me] = full_losses[me]
        loss = loss.astype(bf16)
        gross = jnp.dot(marks[0], loss[0:rows], preferred_element_type=f32) + jnp.dot(
            marks[1], loss[rows : 2 * rows], preferred_element_type=f32
        )
        for o in range(n):
            program_send[o, 1] = gross[o * prog : (o + 1) * prog, :]

    def close(i):
        q = lax.rem(i + lax.div(seat, chunk) * chunk, team)

        @pl.when(lax.rem(i, chunk) == 0)
        def _():
            part_copy(lax.div(q, chunk)).wait_recv()

        at = rows_of(base + q, pol)
        gross = near_acc[rows_of(q, pol), :] + part_recv[q].astype(f32)
        loss = terms(gross, *spread_of(policy_terms, at, width // LANES)).astype(bf16)
        near_losses[rows_of(q, pol), :] = loss

        @pl.when(q != seat)
        def _():
            near_policy_copy(q).start()

        @pl.when(q == seat)
        def _():
            policy_out[:, columns_of(2 * seat)] = loss

    with jax.named_scope("close"):
        loop(0, team, close)

        @pl.when(core != 0)
        def _():
            ascending(lambda d: full_policy_copy(d).start())

    with jax.named_scope("progsend"):
        near_gross = jnp.dot(marks[side], near_losses[...], preferred_element_type=f32)
        for o in range(n):
            program_send[o, 0] = near_gross[o * prog : (o + 1) * prog, :]
        ascending(lambda d: program_copy(d).start())
        program_recv[me] = program_send[me]
    with jax.named_scope("fpolwait"):
        bulk(FULL_POLICY, full_policy.at[pl.ds(0, n - 1)]).wait_recv()
        low = lax.broadcasted_iota(jnp.int32, (pol // 2, width), 1) < width // 2
        for g in range(team):
            left, right = full_policy[g].astype(f32), full_policy[team + g].astype(f32)
            at = slice((2 * g + 1) * width, (2 * g + 2) * width)
            policy_out[: pol // 2, at] = jnp.where(low, left, swap(right)).astype(bf16)
            policy_out[pol // 2 :, at] = jnp.where(low, swap(left), right).astype(bf16)
    with jax.named_scope("sent"):
        bulk(META, meta.at[pl.ds(0, n - 1)]).wait_send()
        bulk(NEAR, near_send.at[pl.ds(0, team - 1)]).wait_send()
        bulk(FULL, full_send.at[pl.ds(0, n - 1)]).wait_send()
        bulk(PART, part_send).wait_send()
        bulk(NEAR_POLICY, near_losses.at[pl.ds(0, rows - pol), :]).wait_send()
        bulk(FULL_POLICY, full_losses.at[pl.ds(0, n - 1)]).wait_send()
        bulk(PROGRAM, program_send.at[pl.ds(0, n - 1)]).wait_send()
    with jax.named_scope("npolwait"):
        bulk(NEAR_POLICY, near_losses.at[pl.ds(0, rows - pol), :]).wait_recv()
    with jax.named_scope("progwait"):
        bulk(PROGRAM, program_recv.at[pl.ds(0, n - 1)]).wait_recv()
    with jax.named_scope("tail"):
        spread = spread_of(program_terms, every, width // LANES)
        low = lax.broadcasted_iota(jnp.int32, (prog, width), 1) < width // 2
        for g in range(team):
            near = program_recv[g, 0] + program_recv[team + g, 0]
            full = jnp.where(low, program_recv[g, 1], swap(program_recv[team + g, 1]))
            at = 2 * g * width
            program_out[:, at : at + width] = terms(near, *spread)
            program_out[:, at + width : at + 2 * width] = terms(full, *spread)


def store(policy, program, policy_out, program_out, sems):
    copies = [
        pltpu.make_async_copy(policy, policy_out, sems.at[0]),
        pltpu.make_async_copy(program, program_out, sems.at[1]),
    ]
    for copy in copies:
        copy.start()
    for copy in copies:
        copy.wait()


def exchange(
    ground_up,
    item_site,
    item_profile,
    site_owner,
    site_slot,
    site_profile,
    policy_owner,
    policy_slot,
    policy_profile,
    program_profile,
    term_table,
):
    n = lax.axis_size("own")
    items, cols = ground_up.shape
    sites = site_profile.shape[0]
    pol = policy_profile.shape[0]
    prog = program_profile.shape[0]
    width = cols // n
    team = n // 2

    def row(v):
        return v.reshape(-1, min(v.size, LANES))

    inputs = [
        row(v)
        for v in (
            item_site,
            item_profile,
            site_owner,
            site_slot,
            site_profile,
            policy_owner,
            policy_slot,
            policy_profile,
            program_profile,
        )
    ] + [term_table.transpose(1, 0, 2)]
    vmemspec = pl.BlockSpec(memory_space=pltpu.VMEM)
    anyspec = pl.BlockSpec(memory_space=pl.ANY)
    dma = pltpu.SemaphoreType.DMA
    held = pl.pallas_call(
        functools.partial(kernel, n, pol, prog),
        out_shape=(
            pltpu.VMEM((pol, cols), bf16),
            pltpu.VMEM((prog, cols), f32),
        ),
        in_specs=[anyspec] * (1 + SMALL),
        out_specs=(vmemspec, vmemspec),
        scratch_shapes=[
            pltpu.VMEM((2 * (items // LANES), LANES), jnp.int32),
            pltpu.VMEM((3, sites), jnp.int32),
            pltpu.VMEM((3, pol), jnp.int32),
            pltpu.VMEM((1, prog), jnp.int32),
            pltpu.VMEM(inputs[-1].shape, f32),
            pltpu.VMEM((team, items, 2 * width), bf16),
            pltpu.VMEM((8, LANES), jnp.int32),
            pltpu.VMEM((LANES, LANES), f32),
            pltpu.VMEM((3, items, LANES), f32),
            pltpu.VMEM((3, sites, LANES), f32),
            pltpu.VMEM((3, n * pol, LANES), f32),
            pltpu.VMEM((3, prog, LANES), f32),
            pltpu.VMEM((sites, items), bf16),
            pltpu.VMEM((n, 2, LANES), jnp.int32),
            pltpu.VMEM((team, sites, width), bf16),
            pltpu.VMEM((team, sites, width), bf16),
            pltpu.VMEM((n, sites // 2, width), bf16),
            pltpu.VMEM((n, sites // 2, width), bf16),
            pltpu.VMEM((team, pol, width), bf16),
            pltpu.VMEM((team, pol, width), bf16),
            pltpu.VMEM((team * pol, width), f32),
            pltpu.VMEM((team * pol, width), bf16),
            pltpu.VMEM((n, pol // 2, width), bf16),
            pltpu.VMEM((n, pol // 2, width), bf16),
            pltpu.VMEM((n, 2, prog, width), f32),
            pltpu.VMEM((n, 2, prog, width), f32),
            pltpu.VMEM((2, n * prog, team * pol), bf16),
            pltpu.VMEM((2, n * pol, team * sites), bf16),
            dma((5,)),
            dma((team,)),
            dma((2,)),
            dma((7,)),
            dma((7,)),
        ],
        compiler_params=pltpu.CompilerParams(collective_id=0, has_side_effects=True),
        name="loss_terms",
    )(ground_up, *inputs)
    held = [pltpu.with_memory_space_constraint(v, pltpu.VMEM) for v in held]
    return pl.pallas_call(
        store,
        out_shape=tuple(jax.ShapeDtypeStruct(v.shape, v.dtype) for v in held),
        in_specs=[vmemspec] * 2,
        out_specs=(anyspec, anyspec),
        scratch_shapes=[dma((2,))],
        name="store_losses",
    )(*held)


def apply_terms(gross_loss, terms_table, tier_index, profile):
    profile_iota = jnp.arange(terms_table.shape[2], dtype=jnp.int32)
    picker = profile[:, None] == profile_iota[None, :]
    deduct = jnp.sum(jnp.where(picker, terms_table[tier_index, 0][None, :], 0.0), axis=1)[:, None]
    ceiling = jnp.sum(jnp.where(picker, terms_table[tier_index, 1][None, :], 0.0), axis=1)[:, None]
    portion = jnp.sum(jnp.where(picker, terms_table[tier_index, 2][None, :], 0.0), axis=1)[:, None]
    return portion * jnp.minimum(jnp.maximum(gross_loss - deduct, 0.0), ceiling)


def pack_rows(values, target_dev, inner_slot, owners, capacity):
    member = (target_dev[:, None] == jnp.arange(owners, dtype=jnp.int32)[None, :]).astype(jnp.int32)
    before = jnp.cumsum(member, axis=0) - member
    position = jnp.sum(before * member, axis=1)
    target = target_dev * capacity + position
    placer = jnp.arange(owners * capacity, dtype=jnp.int32)[:, None] == target[None, :]
    packed = jnp.dot(
        placer.astype(jnp.bfloat16), values, preferred_element_type=jnp.float32
    ).astype(jnp.bfloat16)
    labels = jnp.sum(jnp.where(placer, (inner_slot + 1)[None, :], 0), axis=1) - 1
    return (
        packed.reshape(owners, capacity, values.shape[1]),
        labels.astype(jnp.bfloat16).reshape(owners, capacity),
    )


def sum_rows(received, labels, slot_count):
    flattened = received.reshape(-1, received.shape[2])
    slot_marks = labels.reshape(-1).astype(jnp.int32)
    picker = (jnp.arange(slot_count, dtype=jnp.int32)[:, None] == slot_marks[None, :]).astype(
        jnp.bfloat16
    )
    return jnp.dot(picker, flattened, preferred_element_type=jnp.float32)


def shards(
    ground_up,
    item_site,
    item_profile,
    site_owner,
    site_slot,
    site_profile,
    policy_owner,
    policy_slot,
    policy_profile,
    program_profile,
    term_table,
):
    owners = lax.axis_size("own")
    covered = apply_terms(ground_up.astype(jnp.float32), term_table, 0, item_profile).astype(
        jnp.bfloat16
    )
    site_total = site_profile.shape[0]
    grouping = (jnp.arange(site_total, dtype=jnp.int32)[:, None] == item_site[None, :]).astype(
        jnp.bfloat16
    )
    site_gross = jnp.dot(grouping, covered, preferred_element_type=jnp.float32)
    site_net = apply_terms(site_gross, term_table, 1, site_profile).astype(jnp.bfloat16)
    capacity = 2 * site_total // owners
    packed, labels = pack_rows(site_net, site_owner[:, 0], site_slot, owners, capacity)
    arrived, arrived_labels = (
        lax.all_to_all(packed, "own", split_axis=0, concat_axis=0, tiled=True),
        lax.all_to_all(labels, "own", split_axis=0, concat_axis=0, tiled=True),
    )
    policy_total = policy_profile.shape[0]
    policy_gross = sum_rows(arrived, arrived_labels, policy_total)
    policy_loss = apply_terms(policy_gross, term_table, 2, policy_profile).astype(jnp.bfloat16)
    program_total = program_profile.shape[0]
    program_capacity = 3 * policy_total // owners
    sent_rows, sent_labels = pack_rows(
        policy_loss, policy_owner[:, 0], policy_slot, owners, program_capacity
    )
    got_rows, got_labels = (
        lax.all_to_all(sent_rows, "own", split_axis=0, concat_axis=0, tiled=True),
        lax.all_to_all(sent_labels, "own", split_axis=0, concat_axis=0, tiled=True),
    )
    program_gross = sum_rows(got_rows, got_labels, program_total)
    program_loss = apply_terms(program_gross, term_table, 3, program_profile)
    return (policy_loss, program_loss)


def solution(mesh):
    placed = (
        P("own", "ev"),
        P("own"),
        P("own"),
        P("own", None),
        P("own"),
        P("own"),
        P("own", None),
        P("own"),
        P("own"),
        P("own"),
        P(),
    )

    def body(ground_up, item_site, item_profile, *rest):
        n = lax.axis_size("own")
        items, cols = ground_up.shape
        sites, pol = rest[2].shape[0], rest[5].shape[0]
        prog = rest[6].shape[0]
        fits = cols % (n * LANES) == 0 and items % LANES == 0 and sites == LANES
        fits = fits and 2 * pol <= LANES and pol % 16 == 0 and prog <= 8
        fits = fits and n % 4 == 0 and n & (n - 1) == 0 and 3 * n <= LANES and 3 * items <= LANES * (LANES - 6)
        return (exchange if fits else shards)(ground_up, item_site, item_profile, *rest)

    return jax.shard_map(
        body,
        mesh=mesh,
        in_specs=placed,
        out_specs=(P("own", "ev"), P("own", "ev")),
        check_vma=False,
    )
```
